32 devices in a mesh: dp: 8 (over y, x, core), tensor: 4 (over z).
Axes of the slice: x: 2, y: 2, z: 4, core: 2. Of those that a mesh axis runs over, the one named last changes fastest.
Arguments:
- tokens: bfloat16 [8192, 1536], P(('dp', 'tensor')), may hold values from -6 to 6
- segment_ids: int32 [8, 1024], P('dp'), may hold values from 0 to 3, never falling along the last dimension, each value on 1 to 512 neighbouring positions
- cotangent: bfloat16 [8192, 1536], P(('dp', 'tensor')), may hold values from -6 to 6
- norm_gain: bfloat16 [1536], P(('dp', 'tensor')), may hold values from 0.5 to 1.5
- w_zx: bfloat16 [1536, 2, 3072], P('dp', None, 'tensor'), may hold values from -0.15625 to 0.15625
- w_bc: bfloat16 [1536, 256], P(('dp', 'tensor')), may hold values from -0.15625 to 0.15625
- w_dt: bfloat16 [1536, 48], P('dp', 'tensor'), may hold values from -0.15625 to 0.15625
- conv_x_w: float32 [4, 3072], P(None, 'tensor'), may hold values from -3 to 3
- conv_x_b: float32 [3072], P('tensor'), may hold values from -3 to 3
- conv_bc_w: float32 [4, 256], replicated, may hold values from -3 to 3
- conv_bc_b: float32 [256], replicated, may hold values from -3 to 3
- dt_bias: float32 [48], P('tensor'), may hold values from -6 to -1
- a_log: float32 [48], P('tensor'), may hold values from -4 to 1
- d_skip: float32 [48], P('tensor'), may hold values from 0.5 to 2
- gate_gain: float32 [3072], P('tensor'), may hold values from 0.5 to 1.5
- w_out: bfloat16 [3072, 1536], P('tensor', 'dp'), may hold values from -0.109375 to 0.109375
Outputs:
- layer_out: bfloat16 [8192, 1536], P(('dp', 'tensor'))
- grad_tokens: float32 [8192, 1536], P(('dp', 'tensor'))
- grad_norm_gain: float32 [1536], P(('dp', 'tensor'))
- grad_w_zx: float32 [1536, 2, 3072], P('dp', None, 'tensor')
- grad_w_bc: float32 [1536, 256], P(('dp', 'tensor'))
- grad_w_dt: float32 [1536, 48], P('dp', 'tensor')
- grad_conv_x_w: float32 [4, 3072], P(None, 'tensor')
- grad_conv_x_b: float32 [3072], P('tensor')
- grad_conv_bc_w: float32 [4, 256], replicated
- grad_conv_bc_b: float32 [256], replicated
- grad_dt_bias: float32 [48], P('tensor')
- grad_a_log: float32 [48], P('tensor')
- grad_d_skip: float32 [48], P('tensor')
- grad_gate_gain: float32 [3072], P('tensor')
- grad_w_out: float32 [3072, 1536], P('tensor', 'dp')
The draws below stay inside these ranges and needn't reach their ends.
Inputs may be any that keep to these rules, and one draw needn't show every extreme that they name: `segment_ids`: document numbers start at 0 in each sequence and never fall along it; every document holds 1 to half of 1024 positions, and some document holds exactly that many.
All inputs are finite; a program needn't handle non-finite values.
Results may differ from the reference program's by a relative error of at most 0.012.
Values may be sent and summed in bfloat16 or wider, within the bound.
A program may use at most 192 MiB of HBM per device.

```python
import math
import jax
import jax.numpy as jnp
import numpy as np
from jax import lax

D = 1536
HEADS = 48
HEAD_DIM = 64
STATE = 128
CONV = 4
SEQ_LEN = 1024
INNER = 3072
SEQS = 8
TOKENS = 8192


def block_levels(own_key, dims, cuts, least, top_value):
    def one(axis_at, parts):
        draws = jax.random.uniform(jax.random.fold_in(jax.random.fold_in(own_key, 6), axis_at), (parts,), jnp.float32, least / len(cuts), top_value / len(cuts))
        return jnp.repeat(jnp.exp(draws), dims[axis_at] // parts).reshape((-1,) + (1,) * (len(dims) - axis_at - 1))

    loudness = one(*cuts[0])
    for cut in cuts[1:]:
        loudness = loudness * one(*cut)
    return loudness


def length_profile(number_of, total, reach, skew):
    loads = [(1 << 20) // math.isqrt(grade ** skew) + 1 for grade in range(2, number_of + 1)]
    spare, holding = total - reach - (number_of - 1), [1] * (number_of - 1)
    while spare > 0:
        candidates = [i for i in range(number_of - 1) if holding[i] < reach]
        pool, left = sum([loads[i] for i in candidates]), spare
        for i in candidates:
            more = min(reach - holding[i], max(1, left * loads[i] // pool), spare)
            holding[i] = holding[i] + more
            spare = spare - more
    return np.array([reach] + holding)


def ragged_sizes(own_key, count, total, limit, slope):
    if count == 2:
        one = jax.random.randint(own_key, (), max(1, total - limit), min(limit, total - 1) + 1)
        return jnp.stack([one, total - one])
    tallies = jnp.asarray(length_profile(count, total, limit, slope), jnp.int32)
    couples = (count - 1) // 2
    donor, sink = tallies[1:1 + 2 * couples:2], tallies[2:2 + 2 * couples:2]
    margin = jnp.minimum(donor - 1, limit - sink)
    moved = jax.random.randint(jax.random.fold_in(own_key, 1), (couples,), 0, 1 << 20) % (margin + 1)
    tallies = tallies.at[1:1 + 2 * couples:2].set(donor - moved).at[2:2 + 2 * couples:2].set(sink + moved)
    return tallies[jax.random.permutation(jax.random.fold_in(own_key, 2), count)]


def normal_values(stream_key, shape, scale, reach, split=(), held_as=jnp.bfloat16):
    drawn = scale * jax.random.normal(stream_key, shape, jnp.float32)
    if split:
        drawn = drawn * block_levels(stream_key, shape, split, -0.22, 0.18)
    return jnp.clip(drawn, -reach, reach).astype(held_as)


def setup_inputs(seed: int = 0) -> dict:
    key_of = jax.random.split(jax.random.key(seed), 17)
    tokens = normal_values(key_of[0], (TOKENS, D), 1.0, 6.0, ((0, 32),))
    segment_ids = jax.vmap(lambda own: jnp.searchsorted(jnp.cumsum(ragged_sizes(own, 4, SEQ_LEN, SEQ_LEN // 2, 2)), jnp.arange(SEQ_LEN), side="right"))(jax.random.split(key_of[1], SEQS)).reshape((SEQS, SEQ_LEN)).astype(jnp.int32)
    cotangent = normal_values(key_of[2], (TOKENS, D), 1.0, 6.0, ((0, 32),))
    norm_gain = jnp.clip(1.0 + 0.1 * jax.random.normal(key_of[3], (D,), jnp.float32), 0.5, 1.5).astype(jnp.bfloat16)
    w_zx = normal_values(key_of[4], (D, 2, INNER), D ** -0.5, 0.15625, ((0, 8), (2, 4)))
    w_bc = normal_values(key_of[5], (D, 2 * STATE), D ** -0.5, 0.15625, ((0, 32),))
    w_dt = normal_values(key_of[6], (D, HEADS), D ** -0.5, 0.15625, ((0, 8), (1, 4)))
    conv_x_w = normal_values(key_of[7], (CONV, INNER), 0.5, 3.0, ((1, 4),), jnp.float32)
    conv_x_b = normal_values(key_of[8], (INNER,), 0.3, 3.0, ((0, 4),), jnp.float32)
    conv_bc_w = normal_values(key_of[9], (CONV, 2 * STATE), 0.5, 3.0, (), jnp.float32)
    conv_bc_b = normal_values(key_of[10], (2 * STATE,), 0.3, 3.0, (), jnp.float32)
    dt_bias = jnp.clip(-6.0 + 5.0 * jax.random.uniform(key_of[11], (HEADS,), jnp.float32) ** block_levels(key_of[11], (HEADS,), ((0, 4),), -0.2, 0.2), -6.0, -1.0)
    a_log = jnp.clip(-4.0 + 5.0 * jax.random.uniform(key_of[12], (HEADS,), jnp.float32) ** block_levels(key_of[12], (HEADS,), ((0, 4),), -0.2, 0.2), -4.0, 1.0)
    d_skip = jnp.clip(0.5 + 1.5 * jax.random.uniform(key_of[13], (HEADS,), jnp.float32) ** block_levels(key_of[13], (HEADS,), ((0, 4),), -0.2, 0.2), 0.5, 2.0)
    gate_gain = jnp.clip(1.0 + 0.1 * jax.random.normal(key_of[14], (INNER,), jnp.float32), 0.5, 1.5)
    w_out = normal_values(key_of[15], (INNER, D), INNER ** -0.5, 0.109375, ((0, 4), (1, 8)))
    return dict(tokens=tokens, segment_ids=segment_ids, cotangent=cotangent, norm_gain=norm_gain, w_zx=w_zx, w_bc=w_bc, w_dt=w_dt, conv_x_w=conv_x_w, conv_x_b=conv_x_b, conv_bc_w=conv_bc_w, conv_bc_b=conv_bc_b, dt_bias=dt_bias, a_log=a_log, d_skip=d_skip, gate_gain=gate_gain, w_out=w_out)


EPSILON = 1e-05
HIGHEST = lax.Precision.HIGHEST

def silu_grad(values):
    sigmoid_v = jax.nn.sigmoid(values)
    return sigmoid_v * (1.0 + values * (1.0 - sigmoid_v))

def causal_conv(values, kernel, offset, segment):
    length = values.shape[0]
    width = kernel.shape[0]
    padded = jnp.concatenate([jnp.zeros((width - 1, values.shape[1]), jnp.float32), values], 0)
    seg_pad = jnp.concatenate([jnp.full((width - 1,), -1, jnp.int32), segment], 0)
    summed = jnp.zeros(values.shape, jnp.float32) + offset
    for shift_by in range(width):
        shifted = padded[width - 1 - shift_by:width - 1 - shift_by + length]
        same_doc = (seg_pad[width - 1 - shift_by:width - 1 - shift_by + length] == segment).astype(jnp.float32)
        summed = summed + kernel[shift_by] * shifted * same_doc[:, None]
    return summed

def mixer_sequence(conv_in, bc_act, dt_pre, conv_x_w, conv_x_b, dt_bias, a_log, d_skip, segment):
    length = conv_in.shape[0]
    head_count = dt_pre.shape[1]
    conv_act = jax.nn.silu(causal_conv(conv_in, conv_x_w, conv_x_b, segment)).reshape(length, head_count, HEAD_DIM)
    input_mat = bc_act[:, :STATE]
    output_mat = bc_act[:, STATE:]
    step_size = jax.nn.softplus(dt_pre + dt_bias)
    log_decay = step_size * -jnp.exp(a_log)
    cumulative = jnp.cumsum(log_decay, axis=0).T
    places = jnp.arange(length)
    visible = (places[None, :] <= places[:, None]) & (segment[None, :] == segment[:, None])
    exponent = cumulative[:, :, None] - cumulative[:, None, :]
    decay = jnp.exp(jnp.where(visible[None], exponent, 0.0)) * visible[None].astype(jnp.float32)
    scores = jnp.dot(output_mat, input_mat.T, precision=HIGHEST)
    weighted = conv_act * step_size[:, :, None]
    result = jnp.einsum('hts,shp->thp', decay * scores[None], weighted, precision=HIGHEST)
    result = result + d_skip[:, None] * conv_act
    return result.reshape(length, head_count * HEAD_DIM)

def reference(tokens, segment_ids, cotangent, norm_gain, w_zx, w_bc, w_dt, conv_x_w, conv_x_b, conv_bc_w, conv_bc_b, dt_bias, a_log, d_skip, gate_gain, w_out):
    inner = HEADS * HEAD_DIM
    zx_flat = w_zx.reshape(D, 2 * inner)
    gain_f = norm_gain.astype(jnp.float32)
    token_seq = tokens.reshape(SEQS, SEQ_LEN, D)
    cot_seq = cotangent.reshape(SEQS, SEQ_LEN, D)

    def one_sequence(carry, items):
        rows, segment, d_out = items
        tokens_f = rows.astype(jnp.float32)
        inv_rms = lax.rsqrt(lax.optimization_barrier(jnp.mean(tokens_f * tokens_f, -1, keepdims=True)) + EPSILON)
        normed_in = (tokens_f * inv_rms * gain_f).astype(jnp.bfloat16)
        zx_all = jnp.dot(normed_in, zx_flat, preferred_element_type=jnp.float32)
        gate_pre = zx_all[:, :inner]
        conv_in = zx_all[:, inner:]
        bc_pre = jnp.dot(normed_in, w_bc, preferred_element_type=jnp.float32)
        dt_pre = jnp.dot(normed_in, w_dt, preferred_element_type=jnp.float32)

        def bc_piece(bc_values, kernel, offset):
            return jax.nn.silu(causal_conv(bc_values, kernel, offset, segment))
        bc_act, bc_pull = jax.vjp(bc_piece, bc_pre, conv_bc_w, conv_bc_b)

        def core_piece(conv_vals, bc_vals, dt_vals, kernel, offset, bias_dt, log_rate, skip):
            return mixer_sequence(conv_vals, bc_vals, dt_vals, kernel, offset, bias_dt, log_rate, skip, segment)
        core, core_pull = jax.vjp(core_piece, conv_in, bc_act, dt_pre, conv_x_w, conv_x_b, dt_bias, a_log, d_skip)
        gate_act = jax.nn.silu(gate_pre)
        gated = core * gate_act
        gate_rms = lax.rsqrt(lax.optimization_barrier(jnp.mean(gated * gated, -1, keepdims=True)) + EPSILON)
        normed_out = (gated * gate_rms * gate_gain).astype(jnp.bfloat16)
        mixed = jnp.dot(normed_out, w_out, preferred_element_type=jnp.float32)
        layer_rows = (tokens_f + mixed).astype(jnp.bfloat16)
        d_normed = jnp.dot(d_out, w_out.T, preferred_element_type=jnp.float32)
        g_out = jnp.dot(normed_out.T, d_out, preferred_element_type=jnp.float32)
        inner_dot = lax.optimization_barrier(jnp.sum(gated * gate_gain * d_normed, -1, keepdims=True))
        d_gated = gate_rms * gate_gain * d_normed - gated * (gate_rms * gate_rms * gate_rms) * inner_dot / inner
        g_gate_gain = lax.optimization_barrier(jnp.sum(d_normed * gated * gate_rms, 0))
        d_core = d_gated * gate_act
        d_gate = d_gated * core * silu_grad(gate_pre)
        d_conv_in, d_bc_act, d_dt_pre, g_cxw, g_cxb, g_dtb, g_alog, g_skip = core_pull(d_core)
        d_bc_pre, g_cbw, g_cbb = bc_pull(d_bc_act)
        dz_b = jnp.concatenate([d_gate, d_conv_in], 1).astype(jnp.bfloat16)
        dt_b = d_dt_pre.astype(jnp.bfloat16)
        bc_b = d_bc_pre.astype(jnp.bfloat16)
        d_normed_in = jnp.dot(dz_b, zx_flat.T, preferred_element_type=jnp.float32) + jnp.dot(dt_b, w_dt.T, preferred_element_type=jnp.float32) + jnp.dot(bc_b, w_bc.T, preferred_element_type=jnp.float32)
        g_zx = jnp.dot(normed_in.T, dz_b, preferred_element_type=jnp.float32)
        g_dt = jnp.dot(normed_in.T, dt_b, preferred_element_type=jnp.float32)
        g_bc = jnp.dot(normed_in.T, bc_b, preferred_element_type=jnp.float32)
        g_norm = lax.optimization_barrier(jnp.sum(d_normed_in * tokens_f * inv_rms, 0))
        d_tokens = inv_rms * (gain_f * d_normed_in) - tokens_f * (inv_rms * inv_rms * inv_rms) * lax.optimization_barrier(jnp.mean(tokens_f * gain_f * d_normed_in, -1, keepdims=True))
        grad_rows = d_out.astype(jnp.float32) + d_tokens
        terms = (g_norm, g_zx, g_bc, g_dt, g_cxw, g_cxb, g_cbw, g_cbb, g_dtb, g_alog, g_skip, g_gate_gain, g_out)
        carry = tuple((held + term for held, term in zip(carry, terms)))
        return (carry, (layer_rows, grad_rows))
    start = (jnp.zeros((D,), jnp.float32), jnp.zeros((D, 2 * inner), jnp.float32), jnp.zeros((D, 2 * STATE), jnp.float32), jnp.zeros((D, HEADS), jnp.float32), jnp.zeros((CONV, inner), jnp.float32), jnp.zeros((inner,), jnp.float32), jnp.zeros((CONV, 2 * STATE), jnp.float32), jnp.zeros((2 * STATE,), jnp.float32), jnp.zeros((HEADS,), jnp.float32), jnp.zeros((HEADS,), jnp.float32), jnp.zeros((HEADS,), jnp.float32), jnp.zeros((inner,), jnp.float32), jnp.zeros((inner, D), jnp.float32))
    totals, (layer_seq, grad_seq) = lax.scan(one_sequence, start, (token_seq, segment_ids, cot_seq))
    g_norm, g_zx, g_bc, g_dt, g_cxw, g_cxb, g_cbw, g_cbb, g_dtb, g_alog, g_skip, g_gate_gain, g_out = totals
    return (layer_seq.reshape(TOKENS, D), grad_seq.reshape(TOKENS, D), g_norm, g_zx.reshape(D, 2, inner), g_bc, g_dt, g_cxw, g_cxb, g_cbw, g_cbb, g_dtb, g_alog, g_skip, g_gate_gain, g_out)
```

```python
import functools
import jax
import jax.numpy as jnp
from jax import lax
from jax.experimental import pallas as pl
from jax.experimental.pallas import tpu as pltpu
from jax.sharding import PartitionSpec as P

HEAD_DIM = 64
STATE = 128
CHUNK = 128
LANES = 128
HALO = 8
HIGHEST = lax.Precision.HIGHEST
NEGATIVE = -1e30
F32 = jnp.float32
BF16 = jnp.bfloat16


def mm(a, b, dims=((1,), (0,))):
    return lax.dot_general(a, b, (dims, ((), ())), preferred_element_type=F32)


def mm_exact(a, b, dims=((1,), (0,))):
    return lax.dot_general(a, b, (dims, ((), ())), precision=HIGHEST, preferred_element_type=F32)


NT = ((1,), (1,))
TN = ((0,), (0,))


def spread(per_head, expand):
    high = per_head.astype(BF16)
    rest = per_head - high.astype(F32)
    middle = rest.astype(BF16)
    low = (rest - middle.astype(F32)).astype(BF16)
    return mm(high, expand) + (mm(middle, expand) + mm(low, expand))


def gather_heads(values, expand):
    high = values.astype(BF16)
    low = (values - high.astype(F32)).astype(BF16)
    return mm(high, expand, NT) + mm(low, expand, NT)


def head_expand(width):
    rows = lax.broadcasted_iota(jnp.int32, (LANES, width), 0)
    columns = lax.broadcasted_iota(jnp.int32, (LANES, width), 1)
    lower = rows * HEAD_DIM
    return ((columns >= lower) & (columns < lower + HEAD_DIM)).astype(F32).astype(BF16)


def triangle(size):
    rows = lax.broadcasted_iota(jnp.int32, (size, size), 0)
    columns = lax.broadcasted_iota(jnp.int32, (size, size), 1)
    return rows >= columns


def sigmoid(values):
    return 1.0 / (1.0 + jnp.exp(-values))


def softplus(values):
    return jnp.maximum(values, 0.0) + jnp.log(1.0 + jnp.exp(-jnp.abs(values)))


def conv_chunk(window, meta, taps, offset):
    total = offset + taps[0:1] * window[pl.ds(HALO, CHUNK), :]
    for back in (1, 2, 3):
        total = total + taps[back : back + 1] * (
            window[pl.ds(HALO - back, CHUNK), :] * meta[:, back : back + 1]
        )
    return total


def split_pair(values):
    lane = lax.broadcasted_iota(jnp.int32, values.shape, 1)
    zero = jnp.zeros_like(values)
    return jnp.where(lane < HEAD_DIM, values, zero), jnp.where(lane < HEAD_DIM, zero, values)


def decays(dt_pre, heads, meta, lower):
    step = softplus(dt_pre + heads[5:6, :LANES])
    rate = step * heads[6:7, :LANES]
    cumulative = mm_exact(lower, rate)
    return step, cumulative


def forward_kernel(
    gate_ref, conv_ref, bc_ref, dt_ref, meta_ref, seg_row_ref, params_ref,
    core_ref, gated_ref, states_ref, sum_ref, pre_ref, lanes_ref, save_ref,
    window, state,
):
    width = conv_ref.shape[1]
    chunk = pl.program_id(0)

    @pl.when(chunk == 0)
    def _():
        window[pl.ds(0, HALO), :] = jnp.zeros((HALO, window.shape[1]), F32)
        state[...] = jnp.zeros_like(state)

    @pl.when(chunk > 0)
    def _():
        window[pl.ds(0, HALO), :] = window[pl.ds(CHUNK, HALO), :]

    window[pl.ds(HALO, CHUNK), :width] = conv_ref[...]
    window[pl.ds(HALO, CHUNK), width:] = bc_ref[...]
    meta = meta_ref[...]
    pre = conv_chunk(window, meta, params_ref, params_ref[4:5])
    pre_ref[...] = pre
    act = pre * sigmoid(pre)
    mixer_in = act[:, :width]
    input_mat = act[:, width : width + STATE].astype(BF16)
    output_mat = act[:, width + STATE :].astype(BF16)
    below = triangle(CHUNK)
    lower = below.astype(F32)
    visible = below & (meta[:, 5:6] == seg_row_ref[0])
    step, cumulative = decays(dt_ref[...], params_ref, meta, lower)
    cum_rows = cumulative.T
    last = cumulative[CHUNK - 1 : CHUNK]
    expand = head_expand(width)
    step_l = spread(step, expand)
    from_prev_l = spread(jnp.exp(cumulative) * meta[:, 0:1], expand)
    to_end_l = spread(jnp.exp(last - cumulative) * meta[:, 4:5], expand)
    lanes_ref[:, :width] = step_l
    lanes_ref[:, width : 2 * width] = from_prev_l
    lanes_ref[:, 2 * width :] = to_end_l
    save_ref[:, :LANES] = step
    save_ref[:, LANES:] = cumulative
    passing = from_prev_l[CHUNK - 1 : CHUNK]
    weighted = mixer_in * step_l
    weighted_b = weighted.astype(BF16)
    scores = mm(output_mat, input_mat, NT)
    incoming = state[...]
    incoming_b = incoming.astype(BF16)
    states_ref[0] = incoming_b
    before = mm(output_mat, incoming_b) * from_prev_l
    skipped = params_ref[7:8, :width] * mixer_in
    for pair in range(width // LANES):
        mixed = []
        for head in (2 * pair, 2 * pair + 1):
            gap = cumulative[:, head : head + 1] - cum_rows[head : head + 1, :]
            decay = jnp.exp(jnp.where(visible, gap, NEGATIVE))
            mixed.append((decay * scores).astype(BF16))
        first, second = split_pair(weighted_b[:, pair * LANES : (pair + 1) * LANES])
        within = mm(jnp.concatenate(mixed, 1), jnp.concatenate([first, second], 0))
        lanes = slice(pair * LANES, (pair + 1) * LANES)
        core_ref[:, lanes] = within + before[:, lanes] + skipped[:, lanes]
    state[...] = passing * incoming + mm(input_mat, (weighted * to_end_l).astype(BF16), TN)
    gate = gate_ref[...]
    gated = core_ref[...] * (gate * sigmoid(gate))
    gated_ref[...] = gated
    square = gated * gated
    sum_ref[...] = mm_exact(jnp.ones((8, width), F32), square, NT)


def ssm_forward(projected, bc_pre, meta, seg_row, params):
    length, width = projected.shape[0], params.shape[1] - 2 * STATE
    chunks = length // CHUNK
    row = lambda n, at=0: pl.BlockSpec((CHUNK, n), lambda c: (c, at))
    fixed = lambda a: pl.BlockSpec(a.shape, lambda c: (0,) * a.ndim)
    return pl.pallas_call(
        forward_kernel,
        grid=(chunks,),
        in_specs=[
            row(width), row(width, 1), row(2 * STATE), row(LANES, 2 * width // LANES), row(8),
            pl.BlockSpec((1, 1, CHUNK), lambda c: (c, 0, 0)),
            fixed(params),
        ],
        out_specs=[
            row(width), row(width),
            pl.BlockSpec((1, STATE, width), lambda c: (c, 0, 0)),
            pl.BlockSpec((8, CHUNK), lambda c: (0, c)),
            row(width + 2 * STATE), row(3 * width), row(2 * LANES),
        ],
        out_shape=[
            jax.ShapeDtypeStruct((length, width), F32),
            jax.ShapeDtypeStruct((length, width), F32),
            jax.ShapeDtypeStruct((chunks, STATE, width), BF16),
            jax.ShapeDtypeStruct((8, length), F32),
            jax.ShapeDtypeStruct((length, width + 2 * STATE), F32),
            jax.ShapeDtypeStruct((length, 3 * width), F32),
            jax.ShapeDtypeStruct((length, 2 * LANES), F32),
        ],
        scratch_shapes=[
            pltpu.VMEM((CHUNK + HALO, width + 2 * STATE), F32),
            pltpu.VMEM((STATE, width), F32),
        ],
        name="ssm_forward",
    )(projected, projected, bc_pre, projected, meta, seg_row, params)


def backward_kernel(
    inner,
    gate_ref, conv_ref, halo_ref, bc_ref, bc_halo_ref, dt_ref, meta_ref, meta_next_ref, seg_row_ref,
    params_ref, core_ref, d_normed_ref, rms_ref, dots_ref, states_ref, pre_ref, lanes_ref, save_ref,
    dz_ref, dbc_ref, gconv_ref, ghead_ref, ggain_ref, gskip_ref,
    window, d_window, d_state,
):
    width = conv_ref.shape[1]
    place = pl.program_id(0)
    chunk = pl.num_programs(0) - 1 - place

    @pl.when(place == 0)
    def _():
        d_window[pl.ds(CHUNK, HALO), :] = jnp.zeros((HALO, d_window.shape[1]), F32)
        d_state[...] = jnp.zeros_like(d_state)
        gconv_ref[...] = jnp.zeros_like(gconv_ref)
        ghead_ref[...] = jnp.zeros_like(ghead_ref)
        ggain_ref[...] = jnp.zeros_like(ggain_ref)
        gskip_ref[...] = jnp.zeros_like(gskip_ref)

    @pl.when(place > 0)
    def _():
        d_window[pl.ds(CHUNK, HALO), :] = d_window[pl.ds(0, HALO), :]

    keep_halo = (chunk > 0).astype(F32)
    window[pl.ds(0, HALO), :width] = halo_ref[...] * keep_halo
    window[pl.ds(0, HALO), width:] = bc_halo_ref[...] * keep_halo
    window[pl.ds(HALO, CHUNK), :width] = conv_ref[...]
    window[pl.ds(HALO, CHUNK), width:] = bc_ref[...]
    meta = meta_ref[...]
    pre = pre_ref[...]
    sig = sigmoid(pre)
    act = pre * sig
    slope = sig * (1.0 + pre * (1.0 - sig))
    mixer_in = act[:, :width]
    input_mat = act[:, width : width + STATE].astype(BF16)
    output_mat = act[:, width + STATE :].astype(BF16)
    below = triangle(CHUNK)
    lower = below.astype(F32)
    visible = below & (meta[:, 5:6] == seg_row_ref[0])
    step, cumulative = save_ref[:, :LANES], save_ref[:, LANES:]
    cum_rows = cumulative.T
    expand = head_expand(width)
    step_l = lanes_ref[:, :width]
    from_prev_l = lanes_ref[:, width : 2 * width]
    to_end_l = lanes_ref[:, 2 * width :]
    passing = from_prev_l[CHUNK - 1 : CHUNK]
    weighted = mixer_in * step_l
    weighted_b = weighted.astype(BF16)
    scores = mm(output_mat, input_mat, NT)

    gate_rms = jnp.broadcast_to(rms_ref[...], (8, CHUNK)).T[:, 0:1]
    inner_dot = jnp.broadcast_to(dots_ref[...], (8, CHUNK)).T[:, 0:1]
    gate = gate_ref[...]
    gate_sig = sigmoid(gate)
    gate_act = gate * gate_sig
    core = core_ref[...]
    gated = core * gate_act
    d_normed = d_normed_ref[...]
    d_gated = gate_rms * params_ref[8:9, :width] * d_normed - gated * (
        (gate_rms * gate_rms * gate_rms) * inner_dot / inner
    )
    ggain_ref[0:1] += jnp.sum(d_normed * gated * gate_rms, 0, keepdims=True)
    d_core = d_gated * gate_act
    dz_ref[:, :width] = (d_gated * core * (gate_sig * (1.0 + gate * (1.0 - gate_sig)))).astype(BF16)

    d_core_b = d_core.astype(BF16)
    d_core_r = d_core_b.astype(F32)
    incoming_b = states_ref[0]
    d_outgoing = d_state[...]
    d_outgoing_b = d_outgoing.astype(BF16)
    ended = (weighted * to_end_l).astype(BF16)
    after = mm(input_mat, d_outgoing_b) * to_end_l
    scaled_d = (d_core * from_prev_l).astype(BF16)
    d_output = mm(scaled_d, incoming_b, NT)
    d_input = mm(ended, d_outgoing_b, NT)
    d_scores = jnp.zeros((CHUNK, CHUNK), F32)
    d_weighted_parts = []
    for pair in range(width // LANES):
        lanes = slice(pair * LANES, (pair + 1) * LANES)
        first, second = split_pair(weighted_b[:, lanes])
        d_first, d_second = split_pair(d_core_b[:, lanes])
        both_d = mm(d_core_b[:, lanes], jnp.concatenate([first, second], 0), NT)
        mixed = []
        for side, head in enumerate((2 * pair, 2 * pair + 1)):
            gap = cumulative[:, head : head + 1] - cum_rows[head : head + 1, :]
            decay = jnp.exp(jnp.where(visible, gap, NEGATIVE))
            mixed.append((decay * scores).astype(BF16))
            d_scores = d_scores + both_d[:, side * CHUNK : (side + 1) * CHUNK] * decay
        d_weighted_parts.append(
            mm(jnp.concatenate(mixed, 0), jnp.concatenate([d_first, d_second], 0), TN)
        )
    d_within = jnp.concatenate(d_weighted_parts, 1)
    d_scores_b = d_scores.astype(BF16)
    d_output = d_output + mm(d_scores_b, input_mat)
    d_input = d_input + mm(d_scores_b, output_mat, TN)
    d_weighted = d_within + after

    reached = core - params_ref[7:8, :width] * mixer_in
    near = gather_heads(d_core_r * reached - weighted_b.astype(F32) * d_within, expand)
    far_in = gather_heads(weighted * after, expand)
    carried = jnp.sum(d_outgoing * incoming_b.astype(F32), 0, keepdims=True) * passing
    flow = gather_heads(jnp.broadcast_to(carried, (8, width)), expand)[0:1]
    d_rate = mm_exact(lower, near, TN) + (mm_exact(lower, far_in) - far_in) + flow
    d_step = gather_heads(mixer_in * d_weighted, expand) + d_rate * params_ref[6:7, :LANES]
    slope_dt = sigmoid(dt_ref[...] + params_ref[5:6, :LANES])
    d_dt = d_step * slope_dt
    head_lane = lax.broadcasted_iota(jnp.int32, d_dt.shape, 1) < width // HEAD_DIM
    d_dt = jnp.where(head_lane, d_dt, 0.0)
    dz_ref[:, 2 * width :] = d_dt.astype(BF16)
    ghead_ref[0:1, :LANES] += jnp.sum(d_dt, 0, keepdims=True)
    ghead_ref[0:1, LANES:] += jnp.sum(d_rate * (step * params_ref[6:7, :LANES]), 0, keepdims=True)
    gskip_ref[0:1] += jnp.sum(d_core * mixer_in, 0, keepdims=True)
    d_state[...] = passing * d_outgoing + mm(output_mat, scaled_d, TN)

    d_mixer = d_weighted * step_l + d_core * params_ref[7:8, :width]
    d_pre_x = d_mixer * slope[:, :width]
    d_pre_b = d_input * slope[:, width : width + STATE]
    d_pre_c = d_output * slope[:, width + STATE :]
    d_window[pl.ds(0, CHUNK), :width] = d_pre_x
    d_window[pl.ds(0, CHUNK), width : width + STATE] = d_pre_b
    d_window[pl.ds(0, CHUNK), width + STATE :] = d_pre_c
    d_pre = d_window[pl.ds(0, CHUNK), :]
    gconv_ref[4:5] += jnp.sum(d_pre, 0, keepdims=True)
    gconv_ref[0:1] += jnp.sum(d_pre * window[pl.ds(HALO, CHUNK), :], 0, keepdims=True)
    total = params_ref[0:1] * d_pre
    for back in (1, 2, 3):
        gconv_ref[back : back + 1] += jnp.sum(
            d_pre * (window[pl.ds(HALO - back, CHUNK), :] * meta[:, back : back + 1]), 0, keepdims=True
        )
        total = total + params_ref[back : back + 1] * (
            d_window[pl.ds(back, CHUNK), :] * meta_next_ref[:, back : back + 1]
        )
    dz_ref[:, width : 2 * width] = total[:, :width].astype(BF16)
    dbc_ref[...] = total[:, width:].astype(BF16)


def ssm_backward(
    inner, projected, bc_pre, meta, meta_next, seg_row, params, core, d_normed, rms, dots, states,
    pre, lanes, save,
):
    length, width = core.shape
    chunks = length // CHUNK
    back = lambda c: chunks - 1 - c
    row = lambda n, at=0: pl.BlockSpec((CHUNK, n), lambda c: (back(c), at))
    fixed = lambda a: pl.BlockSpec(a.shape, lambda c: (0,) * a.ndim)
    ahead = lambda n, at=0: pl.BlockSpec(
        (HALO, n), lambda c: (jnp.maximum(back(c) * (CHUNK // HALO) - 1, 0), at)
    )
    whole = lambda *s: pl.BlockSpec(s, lambda c: (0, 0))
    channels = width + 2 * STATE
    return pl.pallas_call(
        functools.partial(backward_kernel, inner),
        grid=(chunks,),
        in_specs=[
            row(width), row(width, 1), ahead(width, 1), row(2 * STATE), ahead(2 * STATE),
            row(LANES, 2 * width // LANES), row(8), row(8),
            pl.BlockSpec((1, 1, CHUNK), lambda c: (back(c), 0, 0)),
            fixed(params),
            row(width), row(width),
            pl.BlockSpec((1, CHUNK), lambda c: (0, back(c))), pl.BlockSpec((1, CHUNK), lambda c: (0, back(c))),
            pl.BlockSpec((1, STATE, width), lambda c: (back(c), 0, 0)),
            row(channels), row(3 * width), row(2 * LANES),
        ],
        out_specs=[
            row(2 * width + LANES), row(2 * STATE),
            whole(8, channels), whole(8, 2 * LANES), whole(8, width), whole(8, width),
        ],
        out_shape=[
            jax.ShapeDtypeStruct((length, 2 * width + LANES), BF16),
            jax.ShapeDtypeStruct((length, 2 * STATE), BF16),
            jax.ShapeDtypeStruct((8, channels), F32),
            jax.ShapeDtypeStruct((8, 2 * LANES), F32),
            jax.ShapeDtypeStruct((8, width), F32),
            jax.ShapeDtypeStruct((8, width), F32),
        ],
        scratch_shapes=[
            pltpu.VMEM((CHUNK + HALO, channels), F32),
            pltpu.VMEM((CHUNK + HALO, channels), F32),
            pltpu.VMEM((STATE, width), F32),
        ],
        name="ssm_backward",
    )(projected, projected, projected, bc_pre, bc_pre, projected, meta, meta_next, seg_row, params,
      core, d_normed, rms, dots, states, pre, lanes, save)


def token_meta(segment):
    length = segment.shape[0]
    chunks = length // CHUNK
    by_chunk = segment.reshape(chunks, CHUNK)
    final = by_chunk[:, -1:]
    ahead = jnp.concatenate([jnp.full((1, 1), -1, jnp.int32), final[:-1]], 0)
    from_prev = (by_chunk == ahead).reshape(length)
    keep_end = (by_chunk == final).reshape(length)
    padded = jnp.concatenate([jnp.full((3,), -1, jnp.int32), segment, jnp.full((3,), -1, jnp.int32)])
    behind = [padded[3 - k : 3 - k + length] == segment for k in (1, 2, 3)]
    after = [padded[3 + k : 3 + k + length] == segment for k in (1, 2, 3)]
    none = jnp.zeros((length,), F32)
    stack = lambda columns: jnp.stack([c.astype(F32) for c in columns], 1)
    meta = stack([from_prev] + behind + [keep_end, segment, none, none])
    meta_next = stack([none] + after + [none] * 4)
    return meta, meta_next, segment.astype(F32).reshape(chunks, 1, CHUNK)


MESH = pl.DeviceIdType.MESH
EPSILON = 1e-05
MIB = 1 << 20


def remote(source, target, send_sem, recv_sem, where):
    return pltpu.make_async_remote_copy(
        src_ref=source, dst_ref=target, send_sem=send_sem, recv_sem=recv_sem, device_id=where, device_id_type=MESH
    )


def rows_at(index, count):
    return pl.ds(pl.multiple_of(index * count, 16), count)


def greet(tensor_size, dp_size):
    line, plane = lax.axis_index("tensor"), lax.axis_index("dp")
    barrier = pltpu.get_barrier_semaphore()
    for step in range(1, tensor_size):
        pl.semaphore_signal(
            barrier, inc=1, device_id={"tensor": lax.rem(line + step, tensor_size)}, device_id_type=MESH
        )
    for step in range(1, dp_size):
        pl.semaphore_signal(barrier, inc=1, device_id={"dp": lax.rem(plane + step, dp_size)}, device_id_type=MESH)
    pl.semaphore_wait(barrier, tensor_size - 1 + dp_size - 1)


def flip(index, offset):
    bit = 1
    while bit <= offset:
        if offset & bit:
            index = index + bit - 2 * bit * lax.rem(index // bit, 2)
        bit *= 2
    return index


def entry_kernel(
    tensor_size, dp_size,
    tok_ref, wa_ref, wo_ref, wb_ref, gain_ref, tok_all, wa_all, wo_all, wb_all, gain_all,
    own_sem, right_send, right_recv, left_send, left_recv,
    plane_send, plane_recv, half_send, half_recv, pass_send, pass_recv, small_send, small_recv,
):
    line, plane = lax.axis_index("tensor"), lax.axis_index("dp")
    core, chip, chips = lax.rem(plane, 2), plane // 2, dp_size // 2
    relay = chips == 4
    direct = (1, 2) if relay else tuple(range(1, chips))
    sibling = {"dp": plane + 1 - 2 * core}
    count = tok_ref.shape[0] // PIECES
    smalls = ((wb_ref, wb_all), (gain_ref, gain_all))
    greet(tensor_size, dp_size)

    def small_out(which, offset):
        source, place = smalls[which]
        return remote(
            source, place.at[plane, line], small_send.at[which, offset], small_recv.at[which, offset],
            {"tensor": lax.rem(line + offset, tensor_size)},
        )

    for which in (0, 1):
        for offset in range(1, tensor_size):
            small_out(which, offset).start()
    own = [
        pltpu.make_async_copy(wb_ref, wb_all.at[plane, line], own_sem.at[0]),
        pltpu.make_async_copy(gain_ref, gain_all.at[plane, line], own_sem.at[1]),
        pltpu.make_async_copy(tok_ref, tok_all.at[rows_at(line, tok_ref.shape[0])], own_sem.at[2]),
        pltpu.make_async_copy(wa_ref, wa_all.at[rows_at(plane, wa_ref.shape[0])], own_sem.at[3]),
        pltpu.make_async_copy(wo_ref, wo_all.at[rows_at(plane, wo_ref.shape[0])], own_sem.at[4]),
    ]

    def token_copy(step, piece, to_right, arriving=False):
        origin = line - step if to_right else line + step
        if arriving:
            origin = origin - 1 if to_right else origin + 1
        origin = jnp.clip(origin, 0, tensor_size - 1)
        place = tok_all.at[rows_at(origin * PIECES + piece, count)]
        source = tok_ref.at[pl.ds(piece * count, count)] if step == 0 and not arriving else place
        neighbour = line + 1 if to_right != arriving else line - 1
        return remote(
            source, place,
            (right_send if to_right else left_send).at[step, piece],
            (right_recv if to_right else left_recv).at[step, piece],
            {"tensor": jnp.clip(neighbour, 0, tensor_size - 1)},
        )

    def sends(step, to_right):
        if to_right:
            return (line - step >= 0) & (line + 1 < tensor_size)
        return (line + step < tensor_size) & (line >= 1)

    def forward_tokens(step):
        for piece in range(PIECES):
            for to_right in (True, False):
                @pl.when(sends(step, to_right))
                def _():
                    if step > 0:
                        token_copy(step - 1, piece, to_right, True).wait_recv()
                    token_copy(step, piece, to_right).start()

    def shard(ref, source):
        rows = source.shape[0]
        return lambda d, half=None: ref.at[
            rows_at(d, rows) if half is None else pl.ds(pl.multiple_of(d * rows + half * (rows // 2), 16), rows // 2)
        ]

    def block(ref):
        n = ref.shape[1] // 2
        return lambda d, half=None: ref.at[d] if half is None else ref.at[d, pl.ds(half * n, n)]

    stacks = [
        (wo_ref, shard(wo_all, wo_ref)),
        (None, block(wb_all)),
        (None, block(gain_all)),
        (wa_ref, shard(wa_all, wa_ref)),
    ]

    def device(offset, side):
        return 2 * flip(chip, offset) + side

    def plane_copy(which, offset):
        source, place = stacks[which]
        return remote(
            place(plane) if source is None else source, place(plane),
            plane_send.at[which, offset], plane_recv.at[which, offset], {"dp": device(offset, core)},
        )

    def plane_arrival(which, offset):
        origin = device(offset, core)
        place = stacks[which][1](origin)
        return remote(place, place, plane_send.at[which, offset], plane_recv.at[which, offset], {"dp": origin})

    def half_copy(which, half):
        place = stacks[which][1](device(half + 1, core), half)
        return remote(
            place, place, half_send.at[which, half], half_recv.at[which, half], {"dp": device(2 - half, core)}
        )

    def half_arrival(which, half):
        place = stacks[which][1](device(3, core), half)
        return remote(
            place, place, half_send.at[which, half], half_recv.at[which, half], {"dp": device(2 - half, core)}
        )

    def pass_copy(which, offset, arriving=False):
        source, place = stacks[which]
        origin = device(offset, 1 - core if arriving else core)
        return remote(
            source if offset == 0 and source is not None and not arriving else place(origin), place(origin),
            pass_send.at[which, offset], pass_recv.at[which, offset], sibling,
        )

    def plane_start(which):
        for offset in direct:
            plane_copy(which, offset).start()

    def plane_next(which):
        for offset in direct:
            plane_arrival(which, offset).wait_recv()
            if relay:
                half_copy(which, offset - 1).start()
            pass_copy(which, offset).start()

    def plane_last(which):
        if relay:
            half_arrival(which, 0).wait_recv()
            half_arrival(which, 1).wait_recv()
            pass_copy(which, 3).start()

    forward_tokens(0)
    plane_start(0)
    for copy in own:
        copy.start()
    own[0].wait()
    own[1].wait()
    for which in (0, 1):
        for offset in range(1, tensor_size):
            small_out(which, offset).wait_recv()
    plane_start(1)
    plane_start(2)
    plane_start(3)
    for which in range(4):
        pass_copy(which, 0).start()
    plane_next(0)
    plane_next(1)
    plane_next(2)
    forward_tokens(1)
    plane_next(3)
    for which in range(3):
        plane_last(which)
    for step in range(2, tensor_size - 1):
        forward_tokens(step)
    plane_last(3)

    for to_right in (True, False):
        for step in range(tensor_size - 1):
            arrives = line - 1 - step >= 0 if to_right else line + 1 + step < tensor_size
            at_end = line + 1 == tensor_size if to_right else line == 0

            @pl.when(arrives & at_end)
            def _():
                for piece in range(PIECES):
                    token_copy(step, piece, to_right, True).wait_recv()

            @pl.when(sends(step, to_right))
            def _():
                for piece in range(PIECES):
                    token_copy(step, piece, to_right).wait_send()

    for which in range(4):
        for offset in range(chips):
            pass_copy(which, offset, True).wait_recv()
            pass_copy(which, offset).wait_send()
        for offset in direct:
            plane_copy(which, offset).wait_send()
        if relay:
            half_copy(which, 0).wait_send()
            half_copy(which, 1).wait_send()
    for which in (0, 1):
        for offset in range(1, tensor_size):
            small_out(which, offset).wait_send()
    for copy in own[2:]:
        copy.wait()


PIECES = 2


def entry(tensor_size, dp_size, tokens, wa, wo, wb, gain):
    vmem = pl.BlockSpec(memory_space=pltpu.VMEM)
    anywhere = pl.BlockSpec(memory_space=pl.ANY)
    dma = pltpu.SemaphoreType.DMA
    chips = dp_size // 2
    return pl.pallas_call(
        functools.partial(entry_kernel, tensor_size, dp_size),
        in_specs=[vmem] * 5,
        out_specs=[anywhere] * 5,
        out_shape=[
            jax.ShapeDtypeStruct((tensor_size * tokens.shape[0], tokens.shape[1]), BF16),
            jax.ShapeDtypeStruct((dp_size * wa.shape[0], wa.shape[1]), BF16),
            jax.ShapeDtypeStruct((dp_size * wo.shape[0], wo.shape[1]), BF16),
            jax.ShapeDtypeStruct((dp_size, tensor_size) + wb.shape, BF16),
            jax.ShapeDtypeStruct((dp_size, tensor_size) + gain.shape, BF16),
        ],
        scratch_shapes=[
            dma((5,)), *[dma((tensor_size, PIECES))] * 4,
            dma((4, chips)), dma((4, chips)), dma((4, 2)), dma((4, 2)), dma((4, chips)), dma((4, chips)),
            dma((2, tensor_size)), dma((2, tensor_size)),
        ],
        compiler_params=pltpu.CompilerParams(collective_id=0, has_side_effects=True),
        name="entry_gather",
    )(tokens, wa, wo, wb, gain)


def stat_kernel(tensor_size, inner, own_ref, out_ref, slots, send_sem, recv_sem):
    line = lax.axis_index("tensor")
    barrier = pltpu.get_barrier_semaphore()
    for offset in range(1, tensor_size):
        pl.semaphore_signal(
            barrier, inc=1, device_id={"tensor": lax.rem(line + offset, tensor_size)}, device_id_type=MESH
        )
    pl.semaphore_wait(barrier, tensor_size - 1)
    copies = [
        remote(
            own_ref, slots.at[offset], send_sem.at[offset], recv_sem.at[offset],
            {"tensor": lax.rem(line + offset, tensor_size)},
        )
        for offset in range(1, tensor_size)
    ]
    for copy in copies:
        copy.start()
    total = own_ref[...]
    for offset, copy in enumerate(copies, 1):
        copy.wait_recv()
        total = total + slots[offset]
    out_ref[...] = total if inner is None else lax.rsqrt(total / inner + EPSILON)
    for copy in copies:
        copy.wait_send()


def stat_sum(tensor_size, inner, own, identity):
    vmem = pl.BlockSpec(memory_space=pltpu.VMEM)
    dma = pltpu.SemaphoreType.DMA
    return pl.pallas_call(
        functools.partial(stat_kernel, tensor_size, inner),
        in_specs=[vmem],
        out_specs=vmem,
        out_shape=jax.ShapeDtypeStruct(own.shape, F32),
        scratch_shapes=[pltpu.VMEM((tensor_size,) + own.shape, F32), dma((tensor_size,)), dma((tensor_size,))],
        compiler_params=pltpu.CompilerParams(collective_id=identity, has_side_effects=True),
        name="dot_sum" if inner is None else "rms_sum",
    )(own)


BAND = 16


def add_rows(target, terms, count):
    def step(index, carry):
        at = pl.multiple_of(index * BAND, BAND)
        total = terms[0](at)
        for term in terms[1:]:
            total = total + term(at)
        target(at, total)
        return carry

    lax.fori_loop(0, count // BAND, step, 0)


def exit_kernel(
    tensor_size, dp_size,
    ga_ref, go_ref, gb_ref, small_ref,
    sa_ref, so_ref, sb_ref, plane_sum_ref, all_sum_ref,
    near_a, near_o, near_b, far_a, far_o, far_b, mid_b, b_slots, pair_ref, plane_slots, line_slots,
    near_send, near_recv, far_send, far_recv,
    b_send, b_recv, plane_send, plane_recv, line_send, line_recv,
):
    line, plane = lax.axis_index("tensor"), lax.axis_index("dp")
    core, chip, chips = lax.rem(plane, 2), plane // 2, dp_size // 2
    relay = chips == 4
    sibling = {"dp": plane + 1 - 2 * core}
    greet(tensor_size, dp_size)

    grads = [(ga_ref, near_a, far_a), (go_ref, near_o, far_o), (gb_ref, near_b, far_b)]
    order = [3, 1, 2, 0] if relay else list(range(1, chips)) + [0]
    arrays = (2, 0, 1)

    def device(offset, side):
        return 2 * flip(chip, offset) + side

    def near_copy(which, offset):
        grad, near, _ = grads[which]
        return remote(
            grad.at[rows_at(device(offset, 1 - core), near.shape[1])], near.at[offset],
            near_send.at[which, offset], near_recv.at[which, offset], sibling,
        )

    def far_copy(which, offset, half, towards):
        _, near, far = grads[which]
        span = pl.ds(half * (near.shape[1] // 2), near.shape[1] // 2)
        return remote(
            near.at[offset, span], far.at[offset, span],
            far_send.at[which, offset, half], far_recv.at[which, offset, half], {"dp": device(towards, core)},
        )

    def small_plane(offset):
        if offset == 0:
            return remote(small_ref, plane_slots.at[0], plane_send.at[0], plane_recv.at[0], sibling)
        return remote(
            pair_ref, plane_slots.at[offset], plane_send.at[offset], plane_recv.at[offset],
            {"dp": device(offset, core)},
        )

    def small_line(offset):
        return remote(
            plane_sum_ref.at[pl.ds(8, 8)], line_slots.at[offset], line_send.at[offset], line_recv.at[offset],
            {"tensor": lax.rem(line + offset, tensor_size)},
        )

    def near_sum(offset):
        owner = device(offset, core)
        for which in arrays:
            grad, near, _ = grads[which]
            near_copy(which, offset).wait_recv()
            base = owner * near.shape[1]

            def both(at, near=near, grad=grad, base=base):
                mine = grad[pl.ds(pl.multiple_of(base + at, BAND), BAND), :]
                return near[offset, pl.ds(at, BAND), :].astype(F32) + mine.astype(F32)

            def put(at, total, near=near):
                near[offset, pl.ds(at, BAND), :] = total.astype(BF16)

            add_rows(put, [both], near.shape[1])

    def merge(offset, half, source):
        for which in arrays:
            _, near, far = grads[which]
            span = near.shape[1] // 2
            far_copy(which, 3, half, source).wait_recv()

            def both(at, near=near, far=far, span=span):
                at = half * span + at
                return near[offset, pl.ds(at, BAND), :].astype(F32) + far[3, pl.ds(at, BAND), :].astype(F32)

            def put(at, total, near=near, span=span):
                near[offset, pl.ds(half * span + at, BAND), :] = total.astype(BF16)

            add_rows(put, [both], span)
            far_copy(which, offset, half, offset).start()

    for which in arrays:
        near_copy(which, order[0]).start()
    small_plane(0).start()
    for offset in order[1:]:
        for which in arrays:
            near_copy(which, offset).start()

    for offset in order[:-1]:
        near_sum(offset)
        for which in arrays:
            if not relay:
                far_copy(which, offset, 0, offset).start()
                far_copy(which, offset, 1, offset).start()
            elif offset == 3:
                far_copy(which, 3, 0, 1).start()
                far_copy(which, 3, 1, 2).start()
            else:
                far_copy(which, offset, offset - 1, offset).start()
        if offset == order[0]:
            small_plane(0).wait_recv()
            pair_ref[...] = small_ref[...] + plane_slots[0]
            for away in range(1, chips):
                small_plane(away).start()
    near_sum(0)
    if relay:
        merge(1, 1, 2)
        merge(2, 0, 1)
    total = pair_ref[...]
    for offset in range(1, chips):
        small_plane(offset).wait_recv()
        total = total + plane_slots[offset]
    plane_sum_ref[...] = total
    for offset in range(1, tensor_size):
        small_line(offset).start()

    direct = (1, 2) if relay else tuple(range(1, chips))
    block = sb_ref.shape[0]
    for which, out in ((2, mid_b), (0, sa_ref), (1, so_ref)):
        _, near, far = grads[which]
        for offset in direct:
            for half in (0, 1):
                far_copy(which, offset, half, offset).wait_recv()
        terms = [lambda at, near=near: near[0, pl.ds(at, BAND), :].astype(F32)] + [
            lambda at, far=far, offset=offset: far[offset, pl.ds(at, BAND), :].astype(F32) for offset in direct
        ]

        def put(at, total, out=out):
            out[pl.ds(at, BAND), :] = total

        add_rows(put, terms, near.shape[1])
        if which == 2:
            b_copies = [
                remote(
                    mid_b.at[rows_at(lax.rem(line + offset, tensor_size), block)], b_slots.at[offset],
                    b_send.at[offset], b_recv.at[offset], {"tensor": lax.rem(line + offset, tensor_size)},
                )
                for offset in range(1, tensor_size)
            ]
            for copy in b_copies:
                copy.start()

    total = plane_sum_ref[8:]
    for offset in range(1, tensor_size):
        small_line(offset).wait_recv()
        total = total + line_slots[offset]
    all_sum_ref[...] = total

    total = mid_b[rows_at(line, block), :]
    for offset, copy in enumerate(b_copies, 1):
        copy.wait_recv()
        total = total + b_slots[offset]
    sb_ref[...] = total

    for which in range(3):
        for offset in range(chips):
            near_copy(which, offset).wait_send()
            if offset:
                for half in (0, 1):
                    towards = offset if offset != 3 or not relay else half + 1
                    far_copy(which, offset, half, towards).wait_send()
    for copy in b_copies:
        copy.wait_send()
    for offset in range(chips):
        small_plane(offset).wait_send()
    for offset in range(1, tensor_size):
        small_line(offset).wait_send()


def leave(tensor_size, dp_size, ga, go, gb, small):
    vmem = pl.BlockSpec(memory_space=pltpu.VMEM)
    dma = pltpu.SemaphoreType.DMA
    chips = dp_size // 2
    ra, ro, rb = (g.shape[0] // dp_size for g in (ga, go, gb))
    block = rb // tensor_size
    slots = lambda n, r, c, t=BF16: pltpu.VMEM((n, r, c), t)
    return pl.pallas_call(
        functools.partial(exit_kernel, tensor_size, dp_size),
        in_specs=[vmem] * 4,
        out_specs=[vmem] * 5,
        out_shape=[
            jax.ShapeDtypeStruct((ra, ga.shape[1]), F32),
            jax.ShapeDtypeStruct((ro, go.shape[1]), F32),
            jax.ShapeDtypeStruct((block, gb.shape[1]), F32),
            jax.ShapeDtypeStruct(small.shape, F32),
            jax.ShapeDtypeStruct((8, small.shape[1]), F32),
        ],
        scratch_shapes=[
            slots(chips, ra, ga.shape[1]), slots(chips, ro, go.shape[1]), slots(chips, rb, gb.shape[1]),
            slots(chips, ra, ga.shape[1]), slots(chips, ro, go.shape[1]), slots(chips, rb, gb.shape[1]),
            pltpu.VMEM((rb, gb.shape[1]), F32), slots(tensor_size, block, gb.shape[1], F32),
            pltpu.VMEM(small.shape, F32), slots(chips, *small.shape, F32), slots(tensor_size, 8, small.shape[1], F32),
            dma((3, chips)), dma((3, chips)), dma((3, chips, 2)), dma((3, chips, 2)),
            dma((tensor_size,)), dma((tensor_size,)), dma((chips,)), dma((chips,)),
            dma((tensor_size,)), dma((tensor_size,)),
        ],
        compiler_params=pltpu.CompilerParams(collective_id=2, has_side_effects=True, vmem_limit_bytes=60 * MIB),
        name="exit_reduce",
    )(ga, go, gb, small)


STEPS = 4


def finish_kernel(
    width, bc_rows,
    tok_ref, cot_ref, gain_ref, mixed_ref, d_own_ref, sa_ref, dt_ref, sb_ref, plane_ref, all_ref,
    layer_ref, dtok_ref, gzx_ref, gbc_ref, gdt_ref, cxw_ref, cxb_ref, cbw_ref, cbb_ref, dtb_ref, alog_ref, skip_ref,
    gate_ref,
):
    gain = gain_ref[...]

    def step(index, carry):
        at = pl.ds(pl.multiple_of(index * BAND, BAND), BAND)
        tokens = tok_ref[at, :].astype(F32)
        layer_ref[at, :] = (tokens + mixed_ref[at, :].astype(F32)).astype(BF16)
        inv = lax.rsqrt(jnp.mean(tokens * tokens, -1, keepdims=True) + EPSILON)
        d_own = d_own_ref[at, :].astype(F32)
        slope = gain * d_own
        dtok_ref[at, :] = cot_ref[at, :].astype(F32) + (
            inv * slope - tokens * (inv * inv * inv) * jnp.mean(tokens * slope, -1, keepdims=True)
        )
        return carry

    lax.fori_loop(0, tok_ref.shape[0] // BAND, step, 0)
    gzx_ref[:, 0, :] = sa_ref[:, :width]
    gzx_ref[:, 1, :] = sa_ref[:, width : 2 * width]

    @pl.when(pl.program_id(0) == 0)
    def _():
        gbc_ref[...] = sb_ref[:bc_rows]
        heads = dtb_ref.shape[1]
        gdt_ref[...] = dt_ref[...].T[:heads]
        cxw_ref[...] = plane_ref[:4, :width]
        cxb_ref[...] = plane_ref[4:5, :width]
        gate_ref[...] = plane_ref[5:6, :width]
        dtb_ref[...] = plane_ref[6:7, :heads]
        alog_ref[...] = plane_ref[6:7, LANES : LANES + heads]
        cbw_ref[...] = all_ref[1:5, : 2 * STATE]
        cbb_ref[...] = all_ref[5:6, : 2 * STATE]
        per_head = gather_heads(jnp.broadcast_to(plane_ref[7:8, :width], (8, width)), head_expand(width))
        skip_ref[...] = per_head[0:1, :heads]


def finish(width, bc_rows, heads, tokens, cotangent, gain, mixed, d_own, sa, sb, plane_sum, all_sum):
    row = lambda a: pl.BlockSpec((a[0] // STEPS,) + a[1:], lambda i: (i,) + (0,) * (len(a) - 1))
    last = lambda a: pl.BlockSpec((a[0], LANES), lambda i: (0, 2 * width // LANES))
    fixed = lambda a: pl.BlockSpec(a, lambda i: (0, 0))
    shapes = [
        (tokens.shape, BF16), (tokens.shape, F32), ((sa.shape[0], 2, width), F32), ((bc_rows, sb.shape[1]), F32),
        ((heads, sa.shape[0]), F32), ((4, width), F32), ((1, width), F32), ((4, 2 * STATE), F32), ((1, 2 * STATE), F32),
        ((1, heads), F32), ((1, heads), F32), ((1, heads), F32), ((1, width), F32),
    ]
    kinds = [row, row, row] + [fixed] * 10
    args = (tokens, cotangent, gain, mixed, d_own, sa, sa, sb, plane_sum, all_sum)
    inputs = [row, row, fixed, row, row, row, last, fixed, fixed, fixed]
    return pl.pallas_call(
        functools.partial(finish_kernel, width, bc_rows),
        grid=(STEPS,),
        in_specs=[kind(a.shape) for kind, a in zip(inputs, args)],
        out_specs=[kind(s[0]) for kind, s in zip(kinds, shapes)],
        out_shape=[jax.ShapeDtypeStruct(*s) for s in shapes],
        compiler_params=pltpu.CompilerParams(vmem_limit_bytes=61 * MIB),
        name="finish",
    )(*args)


def pad_lanes(values, size):
    return jnp.pad(values, [(0, 0)] * (values.ndim - 1) + [(0, size - values.shape[-1])])


def dot(a, b, dims, out=F32):
    return lax.dot_general(a, b, (dims, ((), ())), preferred_element_type=out)


def body(
    tensor_size, dp_size,
    tokens, segment_ids, cotangent, norm_gain, w_zx, w_bc, w_dt, conv_x_w, conv_x_b, conv_bc_w, conv_bc_b,
    dt_bias, a_log, d_skip, gate_gain, w_out,
):
    own_rows, model = tokens.shape
    weight_rows, _, width = w_zx.shape
    heads_here = w_dt.shape[1]
    inner = width * tensor_size
    bc_rows = w_bc.shape[0]
    bc_padded = -(-bc_rows // 16) * 16
    assert segment_ids.shape[0] == 1

    wa = jnp.concatenate([w_zx.reshape(weight_rows, 2 * width), pad_lanes(w_dt, LANES)], 1)
    wo = w_out.T
    wb = jnp.pad(w_bc, ((0, bc_padded - bc_rows), (0, 0)))
    gain_block = jnp.broadcast_to(pad_lanes(norm_gain[None], LANES), (16, LANES))
    tok_all, wa_all, wo_all, wb_all, gain_all = entry(tensor_size, dp_size, tokens, wa, wo, wb, gain_block)
    cot_late, _ = lax.optimization_barrier((cotangent, gain_all))
    d_out = lax.all_gather(cot_late, "tensor", axis=0, tiled=True)

    gain = gain_all[:, :, 0, : norm_gain.shape[0]].reshape(1, model).astype(F32)
    wb_all = wb_all[:, :, :bc_rows].reshape(model, 2 * STATE)
    meta, meta_next, seg_row = token_meta(segment_ids[0])
    channels = width + 2 * STATE
    params = jnp.concatenate(
        [
            jnp.concatenate([conv_x_w, conv_bc_w], 1),
            jnp.concatenate([conv_x_b, conv_bc_b])[None],
            pad_lanes(dt_bias[None], channels),
            pad_lanes(-jnp.exp(a_log)[None], channels),
            pad_lanes(jnp.repeat(d_skip, HEAD_DIM)[None], channels),
            pad_lanes(gate_gain[None], channels),
            jnp.zeros((7, channels), F32),
        ],
        0,
    )

    x_all = tok_all.astype(F32)
    inv_all = lax.rsqrt(jnp.mean(x_all * x_all, -1, keepdims=True) + EPSILON)
    normed_in = (x_all * inv_all * gain).astype(BF16)
    projected = dot(normed_in, wa_all, ((1,), (0,)))
    bc_pre = dot(normed_in, wb_all, ((1,), (0,)))
    core, gated, states, sums, pre, lanes, small_save = ssm_forward(projected, bc_pre, meta, seg_row, params)

    gate_row = gate_gain[None]
    rms = stat_sum(tensor_size, inner, sums[:1], 1)
    normed_out = (gated * rms[0][:, None] * gate_row).astype(BF16)
    mixed = dot(normed_out, wo_all, ((1,), (1,)), BF16)
    mixed_own = lax.psum_scatter(mixed, "tensor", scatter_dimension=0, tiled=True)
    d_out, mixed = lax.optimization_barrier((d_out, mixed))
    d_normed = dot(d_out, wo_all, ((1,), (0,)))
    inner_part = jnp.sum(gated * gate_row * d_normed, -1)[None]
    dots = stat_sum(tensor_size, None, inner_part, 3)

    dz, dbc, gconv, ghead, ggain, gskip = ssm_backward(
        inner, projected, bc_pre, meta, meta_next, seg_row, params, core, d_normed, rms, dots, states, pre, lanes, small_save
    )
    go = dot(d_out, normed_out, ((0,), (0,)), BF16)
    part = (dot(dz, wa_all, ((1,), (1,))) + dot(dbc, wb_all, ((1,), (1,)))).astype(BF16)
    ga = dot(normed_in, dz, ((0,), (0,)), BF16)
    gb = dot(normed_in, dbc, ((0,), (0,)), BF16)
    gb = jnp.pad(
        gb.reshape(dp_size * tensor_size, bc_rows, 2 * STATE), ((0, 0), (0, bc_padded - bc_rows), (0, 0))
    ).reshape(dp_size * tensor_size * bc_padded, 2 * STATE)
    gnorm = jnp.sum(part.astype(F32) * x_all * inv_all, 0)[None]
    packed = jnp.concatenate(
        [
            pad_lanes(gconv[:5, :width], model), pad_lanes(ggain[:1], model), pad_lanes(ghead[:1], model),
            pad_lanes(gskip[:1], model), gnorm, pad_lanes(gconv[:5, width:], model), jnp.zeros((2, model), F32),
        ],
        0,
    )
    d_own = lax.psum_scatter(part, "tensor", scatter_dimension=0, tiled=True)
    ga, part = lax.optimization_barrier((ga, part))
    sa, so, sb, plane_sum, all_sum = leave(tensor_size, dp_size, ga, go, gb, packed)
    layer_out, grad_tokens, gzx, gbc, gdt, cxw, cxb, cbw, cbb, dtb, alog, gsk, ggate = finish(
        width, bc_rows, heads_here, tokens, cotangent, gain, mixed_own, d_own, sa, sb, plane_sum, all_sum
    )
    place = lax.axis_index("dp") * tensor_size + lax.axis_index("tensor")
    own_gain = norm_gain.shape[0]
    return (
        layer_out,
        grad_tokens,
        lax.dynamic_slice(all_sum[0], (place * own_gain,), (own_gain,)),
        gzx, gbc, gdt.T, cxw, cxb[0], cbw, cbb[0], dtb[0], alog[0], gsk[0], ggate[0], so.T,
    )


def solution(mesh):
    in_specs = (
        P(("dp", "tensor"), None),
        P("dp", None),
        P(("dp", "tensor"), None),
        P(("dp", "tensor")),
        P("dp", None, "tensor"),
        P(("dp", "tensor"), None),
        P("dp", "tensor"),
        P(None, "tensor"),
        P("tensor"),
        P(),
        P(),
        P("tensor"),
        P("tensor"),
        P("tensor"),
        P("tensor"),
        P("tensor", "dp"),
    )
    out_specs = (
        P(("dp", "tensor"), None),
        P(("dp", "tensor"), None),
        P(("dp", "tensor")),
        P("dp", None, "tensor"),
        P(("dp", "tensor"), None),
        P("dp", "tensor"),
        P(None, "tensor"),
        P("tensor"),
        P(),
        P(),
        P("tensor"),
        P("tensor"),
        P("tensor"),
        P("tensor"),
        P("tensor", "dp"),
    )
    return jax.shard_map(
        functools.partial(body, mesh.shape["tensor"], mesh.shape["dp"]),
        mesh=mesh, in_specs=in_specs, out_specs=out_specs, check_vma=False,
    )
```

```python
import functools
import jax
import jax.numpy as jnp
from jax import lax
from jax.experimental import pallas as pl
from jax.experimental.pallas import tpu as pltpu
from jax.sharding import PartitionSpec as P

HEAD_DIM = 64
STATE = 128
CHUNK = 128
LANES = 128
HALO = 8
HIGHEST = lax.Precision.HIGHEST
NEGATIVE = -1e30
F32 = jnp.float32
BF16 = jnp.bfloat16


def mm(a, b, dims=((1,), (0,))):
    return lax.dot_general(a, b, (dims, ((), ())), preferred_element_type=F32)


def mm_exact(a, b, dims=((1,), (0,))):
    return lax.dot_general(a, b, (dims, ((), ())), precision=HIGHEST, preferred_element_type=F32)


NT = ((1,), (1,))
TN = ((0,), (0,))


def spread(per_head, expand):
    high = per_head.astype(BF16)
    rest = per_head - high.astype(F32)
    middle = rest.astype(BF16)
    low = (rest - middle.astype(F32)).astype(BF16)
    return mm(high, expand) + (mm(middle, expand) + mm(low, expand))


def gather_heads(values, expand):
    high = values.astype(BF16)
    low = (values - high.astype(F32)).astype(BF16)
    return mm(high, expand, NT) + mm(low, expand, NT)


def head_expand(width):
    rows = lax.broadcasted_iota(jnp.int32, (LANES, width), 0)
    columns = lax.broadcasted_iota(jnp.int32, (LANES, width), 1)
    lower = rows * HEAD_DIM
    return ((columns >= lower) & (columns < lower + HEAD_DIM)).astype(F32).astype(BF16)


def triangle(size):
    rows = lax.broadcasted_iota(jnp.int32, (size, size), 0)
    columns = lax.broadcasted_iota(jnp.int32, (size, size), 1)
    return rows >= columns


def sigmoid(values):
    return 1.0 / (1.0 + jnp.exp(-values))


def softplus(values):
    return jnp.maximum(values, 0.0) + jnp.log(1.0 + jnp.exp(-jnp.abs(values)))


def conv_chunk(window, meta, taps, offset):
    total = offset + taps[0:1] * window[pl.ds(HALO, CHUNK), :]
    for back in (1, 2, 3):
        total = total + taps[back : back + 1] * (
            window[pl.ds(HALO - back, CHUNK), :] * meta[:, back : back + 1]
        )
    return total


def split_pair(values):
    lane = lax.broadcasted_iota(jnp.int32, values.shape, 1)
    zero = jnp.zeros_like(values)
    return jnp.where(lane < HEAD_DIM, values, zero), jnp.where(lane < HEAD_DIM, zero, values)


def decays(dt_pre, heads, meta, lower):
    step = softplus(dt_pre + heads[5:6, :LANES])
    rate = step * heads[6:7, :LANES]
    cumulative = mm_exact(lower, rate)
    return step, cumulative


def forward_kernel(
    gate_ref, conv_ref, bc_ref, dt_ref, meta_ref, seg_row_ref, params_ref,
    core_ref, gated_ref, states_ref, sum_ref, pre_ref, lanes_ref, save_ref,
    window, state,
):
    width = conv_ref.shape[1]
    chunk = pl.program_id(0)

    @pl.when(chunk == 0)
    def _():
        window[pl.ds(0, HALO), :] = jnp.zeros((HALO, window.shape[1]), F32)
        state[...] = jnp.zeros_like(state)

    @pl.when(chunk > 0)
    def _():
        window[pl.ds(0, HALO), :] = window[pl.ds(CHUNK, HALO), :]

    window[pl.ds(HALO, CHUNK), :width] = conv_ref[...]
    window[pl.ds(HALO, CHUNK), width:] = bc_ref[...]
    meta = meta_ref[...]
    pre = conv_chunk(window, meta, params_ref, params_ref[4:5])
    pre_ref[...] = pre
    act = pre * sigmoid(pre)
    mixer_in = act[:, :width]
    input_mat = act[:, width : width + STATE].astype(BF16)
    output_mat = act[:, width + STATE :].astype(BF16)
    below = triangle(CHUNK)
    lower = below.astype(F32)
    visible = below & (meta[:, 5:6] == seg_row_ref[0])
    step, cumulative = decays(dt_ref[...], params_ref, meta, lower)
    cum_rows = cumulative.T
    last = cumulative[CHUNK - 1 : CHUNK]
    expand = head_expand(width)
    step_l = spread(step, expand)
    from_prev_l = spread(jnp.exp(cumulative) * meta[:, 0:1], expand)
    to_end_l = spread(jnp.exp(last - cumulative) * meta[:, 4:5], expand)
    lanes_ref[:, :width] = step_l
    lanes_ref[:, width : 2 * width] = from_prev_l
    lanes_ref[:, 2 * width :] = to_end_l
    save_ref[:, :LANES] = step
    save_ref[:, LANES:] = cumulative
    passing = from_prev_l[CHUNK - 1 : CHUNK]
    weighted = mixer_in * step_l
    weighted_b = weighted.astype(BF16)
    scores = mm(output_mat, input_mat, NT)
    incoming = state[...]
    incoming_b = incoming.astype(BF16)
    states_ref[0] = incoming_b
    before = mm(output_mat, incoming_b) * from_prev_l
    skipped = params_ref[7:8, :width] * mixer_in
    for pair in range(width // LANES):
        mixed = []
        for head in (2 * pair, 2 * pair + 1):
            gap = cumulative[:, head : head + 1] - cum_rows[head : head + 1, :]
            decay = jnp.exp(jnp.where(visible, gap, NEGATIVE))
            mixed.append((decay * scores).astype(BF16))
        first, second = split_pair(weighted_b[:, pair * LANES : (pair + 1) * LANES])
        within = mm(jnp.concatenate(mixed, 1), jnp.concatenate([first, second], 0))
        lanes = slice(pair * LANES, (pair + 1) * LANES)
        core_ref[:, lanes] = within + before[:, lanes] + skipped[:, lanes]
    state[...] = passing * incoming + mm(input_mat, (weighted * to_end_l).astype(BF16), TN)
    gate = gate_ref[...]
    gated = core_ref[...] * (gate * sigmoid(gate))
    gated_ref[...] = gated
    square = gated * gated
    sum_ref[...] = mm_exact(jnp.ones((8, width), F32), square, NT)


def ssm_forward(projected, bc_pre, meta, seg_row, params):
    length, width = projected.shape[0], params.shape[1] - 2 * STATE
    chunks = length // CHUNK
    row = lambda n, at=0: pl.BlockSpec((CHUNK, n), lambda c: (c, at))
    fixed = lambda a: pl.BlockSpec(a.shape, lambda c: (0,) * a.ndim)
    return pl.pallas_call(
        forward_kernel,
        grid=(chunks,),
        in_specs=[
            row(width), row(width, 1), row(2 * STATE), row(LANES, 2 * width // LANES), row(8),
            pl.BlockSpec((1, 1, CHUNK), lambda c: (c, 0, 0)),
            fixed(params),
        ],
        out_specs=[
            row(width), row(width),
            pl.BlockSpec((1, STATE, width), lambda c: (c, 0, 0)),
            pl.BlockSpec((8, CHUNK), lambda c: (0, c)),
            row(width + 2 * STATE), row(3 * width), row(2 * LANES),
        ],
        out_shape=[
            jax.ShapeDtypeStruct((length, width), F32),
            jax.ShapeDtypeStruct((length, width), F32),
            jax.ShapeDtypeStruct((chunks, STATE, width), BF16),
            jax.ShapeDtypeStruct((8, length), F32),
            jax.ShapeDtypeStruct((length, width + 2 * STATE), F32),
            jax.ShapeDtypeStruct((length, 3 * width), F32),
            jax.ShapeDtypeStruct((length, 2 * LANES), F32),
        ],
        scratch_shapes=[
            pltpu.VMEM((CHUNK + HALO, width + 2 * STATE), F32),
            pltpu.VMEM((STATE, width), F32),
        ],
        name="ssm_forward",
    )(projected, projected, bc_pre, projected, meta, seg_row, params)


def backward_kernel(
    inner,
    gate_ref, conv_ref, halo_ref, bc_ref, bc_halo_ref, dt_ref, meta_ref, meta_next_ref, seg_row_ref,
    params_ref, core_ref, d_normed_ref, rms_ref, dots_ref, states_ref, pre_ref, lanes_ref, save_ref,
    dz_ref, packed_ref,
    window, d_window, d_state,
):
    width = conv_ref.shape[1]
    place = pl.program_id(0)
    chunk = pl.num_programs(0) - 1 - place

    @pl.when(place == 0)
    def _():
        d_window[pl.ds(CHUNK, HALO), :] = jnp.zeros((HALO, d_window.shape[1]), F32)
        d_state[...] = jnp.zeros_like(d_state)
        packed_ref[...] = jnp.zeros_like(packed_ref)

    @pl.when(place > 0)
    def _():
        d_window[pl.ds(CHUNK, HALO), :] = d_window[pl.ds(0, HALO), :]

    keep_halo = (chunk > 0).astype(F32)
    window[pl.ds(0, HALO), :width] = halo_ref[...] * keep_halo
    window[pl.ds(0, HALO), width:] = bc_halo_ref[...] * keep_halo
    window[pl.ds(HALO, CHUNK), :width] = conv_ref[...]
    window[pl.ds(HALO, CHUNK), width:] = bc_ref[...]
    meta = meta_ref[...]
    pre = pre_ref[...]
    sig = sigmoid(pre)
    act = pre * sig
    slope = sig * (1.0 + pre * (1.0 - sig))
    mixer_in = act[:, :width]
    input_mat = act[:, width : width + STATE].astype(BF16)
    output_mat = act[:, width + STATE :].astype(BF16)
    below = triangle(CHUNK)
    lower = below.astype(F32)
    visible = below & (meta[:, 5:6] == seg_row_ref[0])
    step, cumulative = save_ref[:, :LANES], save_ref[:, LANES:]
    cum_rows = cumulative.T
    expand = head_expand(width)
    step_l = lanes_ref[:, :width]
    from_prev_l = lanes_ref[:, width : 2 * width]
    to_end_l = lanes_ref[:, 2 * width :]
    passing = from_prev_l[CHUNK - 1 : CHUNK]
    weighted = mixer_in * step_l
    weighted_b = weighted.astype(BF16)
    scores = mm(output_mat, input_mat, NT)

    gate_rms = jnp.broadcast_to(rms_ref[...], (8, CHUNK)).T[:, 0:1]
    inner_dot = jnp.broadcast_to(dots_ref[...], (8, CHUNK)).T[:, 0:1]
    gate = gate_ref[...]
    gate_sig = sigmoid(gate)
    gate_act = gate * gate_sig
    core = core_ref[...]
    gated = core * gate_act
    d_normed = d_normed_ref[...]
    d_gated = gate_rms * params_ref[8:9, :width] * d_normed - gated * (
        (gate_rms * gate_rms * gate_rms) * inner_dot / inner
    )
    packed_ref[5:6, :width] += jnp.sum(d_normed * gated * gate_rms, 0, keepdims=True)
    d_core = d_gated * gate_act
    dz_ref[:, :width] = (d_gated * core * (gate_sig * (1.0 + gate * (1.0 - gate_sig)))).astype(BF16)

    d_core_b = d_core.astype(BF16)
    d_core_r = d_core_b.astype(F32)
    incoming_b = states_ref[0]
    d_outgoing = d_state[...]
    d_outgoing_b = d_outgoing.astype(BF16)
    ended = (weighted * to_end_l).astype(BF16)
    after = mm(input_mat, d_outgoing_b) * to_end_l
    scaled_d = (d_core * from_prev_l).astype(BF16)
    d_output = mm(scaled_d, incoming_b, NT)
    d_input = mm(ended, d_outgoing_b, NT)
    d_scores = jnp.zeros((CHUNK, CHUNK), F32)
    d_weighted_parts = []
    for pair in range(width // LANES):
        lanes = slice(pair * LANES, (pair + 1) * LANES)
        first, second = split_pair(weighted_b[:, lanes])
        d_first, d_second = split_pair(d_core_b[:, lanes])
        both_d = mm(d_core_b[:, lanes], jnp.concatenate([first, second], 0), NT)
        mixed = []
        for side, head in enumerate((2 * pair, 2 * pair + 1)):
            gap = cumulative[:, head : head + 1] - cum_rows[head : head + 1, :]
            decay = jnp.exp(jnp.where(visible, gap, NEGATIVE))
            mixed.append((decay * scores).astype(BF16))
            d_scores = d_scores + both_d[:, side * CHUNK : (side + 1) * CHUNK] * decay
        d_weighted_parts.append(
            mm(jnp.concatenate(mixed, 0), jnp.concatenate([d_first, d_second], 0), TN)
        )
    d_within = jnp.concatenate(d_weighted_parts, 1)
    d_scores_b = d_scores.astype(BF16)
    d_output = d_output + mm(d_scores_b, input_mat)
    d_input = d_input + mm(d_scores_b, output_mat, TN)
    d_weighted = d_within + after

    reached = core - params_ref[7:8, :width] * mixer_in
    near = gather_heads(d_core_r * reached - weighted_b.astype(F32) * d_within, expand)
    far_in = gather_heads(weighted * after, expand)
    carried = jnp.sum(d_outgoing * incoming_b.astype(F32), 0, keepdims=True) * passing
    flow = gather_heads(jnp.broadcast_to(carried, (8, width)), expand)[0:1]
    d_rate = mm_exact(lower, near, TN) + (mm_exact(lower, far_in) - far_in) + flow
    d_step = gather_heads(mixer_in * d_weighted, expand) + d_rate * params_ref[6:7, :LANES]
    slope_dt = sigmoid(dt_ref[...] + params_ref[5:6, :LANES])
    d_dt = d_step * slope_dt
    head_lane = lax.broadcasted_iota(jnp.int32, d_dt.shape, 1) < width // HEAD_DIM
    d_dt = jnp.where(head_lane, d_dt, 0.0)
    dz_ref[:, 2 * width : 2 * width + LANES] = d_dt.astype(BF16)
    packed_ref[6:7, :LANES] += jnp.sum(d_dt, 0, keepdims=True)
    packed_ref[6:7, LANES : 2 * LANES] += jnp.sum(d_rate * (step * params_ref[6:7, :LANES]), 0, keepdims=True)
    packed_ref[7:8, :width] += jnp.sum(d_core * mixer_in, 0, keepdims=True)
    d_state[...] = passing * d_outgoing + mm(output_mat, scaled_d, TN)

    d_mixer = d_weighted * step_l + d_core * params_ref[7:8, :width]
    d_pre_x = d_mixer * slope[:, :width]
    d_pre_b = d_input * slope[:, width : width + STATE]
    d_pre_c = d_output * slope[:, width + STATE :]
    d_window[pl.ds(0, CHUNK), :width] = d_pre_x
    d_window[pl.ds(0, CHUNK), width : width + STATE] = d_pre_b
    d_window[pl.ds(0, CHUNK), width + STATE :] = d_pre_c
    d_pre = d_window[pl.ds(0, CHUNK), :]
    taps_seen = [jnp.sum(d_pre * window[pl.ds(HALO, CHUNK), :], 0, keepdims=True)]
    total = params_ref[0:1] * d_pre
    for back in (1, 2, 3):
        taps_seen.append(
            jnp.sum(d_pre * (window[pl.ds(HALO - back, CHUNK), :] * meta[:, back : back + 1]), 0, keepdims=True)
        )
        total = total + params_ref[back : back + 1] * (
            d_window[pl.ds(back, CHUNK), :] * meta_next_ref[:, back : back + 1]
        )
    dz_ref[:, width : 2 * width] = total[:, :width].astype(BF16)
    dz_ref[:, 2 * width + LANES :] = total[:, width:].astype(BF16)
    taps_seen.append(jnp.sum(d_pre, 0, keepdims=True))
    for place_at, seen in enumerate(taps_seen):
        packed_ref[place_at : place_at + 1, :width] += seen[:, :width]
        packed_ref[9 + place_at : 10 + place_at, : 2 * STATE] += seen[:, width:]


def ssm_backward(
    inner, projected, bc_pre, meta, meta_next, seg_row, params, core, d_normed, rms, dots, states,
    pre, lanes, save, model,
):
    length, width = core.shape
    chunks = length // CHUNK
    back = lambda c: chunks - 1 - c
    row = lambda n, at=0: pl.BlockSpec((CHUNK, n), lambda c: (back(c), at))
    fixed = lambda a: pl.BlockSpec(a.shape, lambda c: (0,) * a.ndim)
    ahead = lambda n, at=0: pl.BlockSpec(
        (HALO, n), lambda c: (jnp.maximum(back(c) * (CHUNK // HALO) - 1, 0), at)
    )
    whole = lambda *s: pl.BlockSpec(s, lambda c: (0, 0))
    channels = width + 2 * STATE
    return pl.pallas_call(
        functools.partial(backward_kernel, inner),
        grid=(chunks,),
        in_specs=[
            row(width), row(width, 1), ahead(width, 1), row(2 * STATE), ahead(2 * STATE),
            row(LANES, 2 * width // LANES), row(8), row(8),
            pl.BlockSpec((1, 1, CHUNK), lambda c: (back(c), 0, 0)),
            fixed(params),
            row(width), row(width),
            pl.BlockSpec((1, CHUNK), lambda c: (0, back(c))), pl.BlockSpec((1, CHUNK), lambda c: (0, back(c))),
            pl.BlockSpec((1, STATE, width), lambda c: (back(c), 0, 0)),
            row(channels), row(3 * width), row(2 * LANES),
        ],
        out_specs=[
            row(2 * width + LANES + 2 * STATE), whole(16, model),
        ],
        out_shape=[
            jax.ShapeDtypeStruct((length, 2 * width + LANES + 2 * STATE), BF16),
            jax.ShapeDtypeStruct((16, model), F32),
        ],
        scratch_shapes=[
            pltpu.VMEM((CHUNK + HALO, channels), F32),
            pltpu.VMEM((CHUNK + HALO, channels), F32),
            pltpu.VMEM((STATE, width), F32),
        ],
        name="ssm_backward",
    )(projected, projected, projected, bc_pre, bc_pre, projected, meta, meta_next, seg_row, params,
      core, d_normed, rms, dots, states, pre, lanes, save)


def token_meta(segment):
    length = segment.shape[0]
    chunks = length // CHUNK
    by_chunk = segment.reshape(chunks, CHUNK)
    final = by_chunk[:, -1:]
    ahead = jnp.concatenate([jnp.full((1, 1), -1, jnp.int32), final[:-1]], 0)
    from_prev = (by_chunk == ahead).reshape(length)
    keep_end = (by_chunk == final).reshape(length)
    padded = jnp.concatenate([jnp.full((3,), -1, jnp.int32), segment, jnp.full((3,), -1, jnp.int32)])
    behind = [padded[3 - k : 3 - k + length] == segment for k in (1, 2, 3)]
    after = [padded[3 + k : 3 + k + length] == segment for k in (1, 2, 3)]
    none = jnp.zeros((length,), F32)
    stack = lambda columns: jnp.stack([c.astype(F32) for c in columns], 1)
    meta = stack([from_prev] + behind + [keep_end, segment, none, none])
    meta_next = stack([none] + after + [none] * 4)
    return meta, meta_next, segment.astype(F32).reshape(chunks, 1, CHUNK)


MESH = pl.DeviceIdType.MESH
EPSILON = 1e-05
MIB = 1 << 20


def remote(source, target, send_sem, recv_sem, where):
    return pltpu.make_async_remote_copy(
        src_ref=source, dst_ref=target, send_sem=send_sem, recv_sem=recv_sem, device_id=where, device_id_type=MESH
    )


def rows_at(index, count):
    return pl.ds(pl.multiple_of(index * count, 16), count)


def greet(tensor_size, dp_size):
    line, plane = lax.axis_index("tensor"), lax.axis_index("dp")
    barrier = pltpu.get_barrier_semaphore()
    for step in range(1, tensor_size):
        pl.semaphore_signal(
            barrier, inc=1, device_id={"tensor": lax.rem(line + step, tensor_size)}, device_id_type=MESH
        )
    for step in range(1, dp_size):
        pl.semaphore_signal(barrier, inc=1, device_id={"dp": lax.rem(plane + step, dp_size)}, device_id_type=MESH)
    pl.semaphore_wait(barrier, tensor_size - 1 + dp_size - 1)


def flip(index, offset):
    bit = 1
    while bit <= offset:
        if offset & bit:
            index = index + bit - 2 * bit * lax.rem(index // bit, 2)
        bit *= 2
    return index


def entry_kernel(
    tensor_size, dp_size,
    tok_ref, wa_ref, wo_ref, wb_ref, gain_ref, tok_all, wa_all, wo_all, wb_all, gain_all,
    own_sem, right_send, right_recv, left_send, left_recv,
    plane_send, plane_recv, half_send, half_recv, pass_send, pass_recv, small_send, small_recv,
):
    line, plane = lax.axis_index("tensor"), lax.axis_index("dp")
    core, chip, chips = lax.rem(plane, 2), plane // 2, dp_size // 2
    relay = chips == 4
    direct = (1, 2) if relay else tuple(range(1, chips))
    sibling = {"dp": plane + 1 - 2 * core}
    count = tok_ref.shape[0] // PIECES
    smalls = ((wb_ref, wb_all), (gain_ref, gain_all))
    greet(tensor_size, dp_size)

    def small_out(which, offset):
        source, place = smalls[which]
        return remote(
            source, place.at[plane, line], small_send.at[which, offset], small_recv.at[which, offset],
            {"tensor": lax.rem(line + offset, tensor_size)},
        )

    for which in (0, 1):
        for offset in range(1, tensor_size):
            small_out(which, offset).start()
    own = [
        pltpu.make_async_copy(wb_ref, wb_all.at[plane, line], own_sem.at[0]),
        pltpu.make_async_copy(gain_ref, gain_all.at[plane, line], own_sem.at[1]),
        pltpu.make_async_copy(tok_ref, tok_all.at[rows_at(line, tok_ref.shape[0])], own_sem.at[2]),
        pltpu.make_async_copy(wa_ref, wa_all.at[rows_at(plane, wa_ref.shape[0])], own_sem.at[3]),
        pltpu.make_async_copy(wo_ref, wo_all.at[rows_at(plane, wo_ref.shape[0])], own_sem.at[4]),
    ]

    def token_copy(step, piece, to_right, arriving=False):
        origin = line - step if to_right else line + step
        if arriving:
            origin = origin - 1 if to_right else origin + 1
        origin = jnp.clip(origin, 0, tensor_size - 1)
        place = tok_all.at[rows_at(origin * PIECES + piece, count)]
        source = tok_ref.at[pl.ds(piece * count, count)] if step == 0 and not arriving else place
        neighbour = line + 1 if to_right != arriving else line - 1
        return remote(
            source, place,
            (right_send if to_right else left_send).at[step, piece],
            (right_recv if to_right else left_recv).at[step, piece],
            {"tensor": jnp.clip(neighbour, 0, tensor_size - 1)},
        )

    def sends(step, to_right):
        if to_right:
            return (line - step >= 0) & (line + 1 < tensor_size)
        return (line + step < tensor_size) & (line >= 1)

    def forward_tokens(step):
        for piece in range(PIECES):
            for to_right in (True, False):
                @pl.when(sends(step, to_right))
                def _():
                    if step > 0:
                        token_copy(step - 1, piece, to_right, True).wait_recv()
                    token_copy(step, piece, to_right).start()

    def shard(ref, source):
        rows = source.shape[0]
        return lambda d, half=None: ref.at[
            rows_at(d, rows) if half is None else pl.ds(pl.multiple_of(d * rows + half * (rows // 2), 16), rows // 2)
        ]

    def block(ref):
        n = ref.shape[1] // 2
        return lambda d, half=None: ref.at[d] if half is None else ref.at[d, pl.ds(half * n, n)]

    stacks = [
        (wo_ref, shard(wo_all, wo_ref)),
        (None, block(wb_all)),
        (None, block(gain_all)),
        (wa_ref, shard(wa_all, wa_ref)),
    ]

    def device(offset, side):
        return 2 * flip(chip, offset) + side

    def plane_copy(which, offset):
        source, place = stacks[which]
        return remote(
            place(plane) if source is None else source, place(plane),
            plane_send.at[which, offset], plane_recv.at[which, offset], {"dp": device(offset, core)},
        )

    def plane_arrival(which, offset):
        origin = device(offset, core)
        place = stacks[which][1](origin)
        return remote(place, place, plane_send.at[which, offset], plane_recv.at[which, offset], {"dp": origin})

    def half_copy(which, half):
        place = stacks[which][1](device(half + 1, core), half)
        return remote(
            place, place, half_send.at[which, half], half_recv.at[which, half], {"dp": device(2 - half, core)}
        )

    def half_arrival(which, half):
        place = stacks[which][1](device(3, core), half)
        return remote(
            place, place, half_send.at[which, half], half_recv.at[which, half], {"dp": device(2 - half, core)}
        )

    def pass_copy(which, offset, arriving=False):
        source, place = stacks[which]
        origin = device(offset, 1 - core if arriving else core)
        return remote(
            source if offset == 0 and source is not None and not arriving else place(origin), place(origin),
            pass_send.at[which, offset], pass_recv.at[which, offset], sibling,
        )

    def plane_start(which):
        for offset in direct:
            plane_copy(which, offset).start()

    def plane_next(which):
        for offset in direct:
            plane_arrival(which, offset).wait_recv()
            if relay:
                half_copy(which, offset - 1).start()
            pass_copy(which, offset).start()

    def plane_last(which):
        if relay:
            half_arrival(which, 0).wait_recv()
            half_arrival(which, 1).wait_recv()
            pass_copy(which, 3).start()

    forward_tokens(0)
    plane_start(0)
    for copy in own:
        copy.start()
    own[0].wait()
    own[1].wait()
    for which in (0, 1):
        for offset in range(1, tensor_size):
            small_out(which, offset).wait_recv()
    plane_start(1)
    plane_start(2)
    plane_start(3)
    for which in range(4):
        pass_copy(which, 0).start()
    plane_next(0)
    plane_next(1)
    plane_next(2)
    forward_tokens(1)
    plane_next(3)
    for which in range(3):
        plane_last(which)
    for step in range(2, tensor_size - 1):
        forward_tokens(step)
    plane_last(3)

    for to_right in (True, False):
        for step in range(tensor_size - 1):
            arrives = line - 1 - step >= 0 if to_right else line + 1 + step < tensor_size
            at_end = line + 1 == tensor_size if to_right else line == 0

            @pl.when(arrives & at_end)
            def _():
                for piece in range(PIECES):
                    token_copy(step, piece, to_right, True).wait_recv()

            @pl.when(sends(step, to_right))
            def _():
                for piece in range(PIECES):
                    token_copy(step, piece, to_right).wait_send()

    for which in range(4):
        for offset in range(chips):
            pass_copy(which, offset, True).wait_recv()
            pass_copy(which, offset).wait_send()
        for offset in direct:
            plane_copy(which, offset).wait_send()
        if relay:
            half_copy(which, 0).wait_send()
            half_copy(which, 1).wait_send()
    for which in (0, 1):
        for offset in range(1, tensor_size):
            small_out(which, offset).wait_send()
    for copy in own[2:]:
        copy.wait()


PIECES = 2


def entry(tensor_size, dp_size, tokens, wa, wo, wb, gain):
    vmem = pl.BlockSpec(memory_space=pltpu.VMEM)
    anywhere = pl.BlockSpec(memory_space=pl.ANY)
    dma = pltpu.SemaphoreType.DMA
    chips = dp_size // 2
    return pl.pallas_call(
        functools.partial(entry_kernel, tensor_size, dp_size),
        in_specs=[vmem] * 5,
        out_specs=[anywhere] * 5,
        out_shape=[
            jax.ShapeDtypeStruct((tensor_size * tokens.shape[0], tokens.shape[1]), BF16),
            jax.ShapeDtypeStruct((dp_size * wa.shape[0], wa.shape[1]), BF16),
            jax.ShapeDtypeStruct((dp_size * wo.shape[0], wo.shape[1]), BF16),
            jax.ShapeDtypeStruct((dp_size, tensor_size) + wb.shape, BF16),
            jax.ShapeDtypeStruct((dp_size, tensor_size) + gain.shape, BF16),
        ],
        scratch_shapes=[
            dma((5,)), *[dma((tensor_size, PIECES))] * 4,
            dma((4, chips)), dma((4, chips)), dma((4, 2)), dma((4, 2)), dma((4, chips)), dma((4, chips)),
            dma((2, tensor_size)), dma((2, tensor_size)),
        ],
        compiler_params=pltpu.CompilerParams(collective_id=0, has_side_effects=True),
        name="entry_gather",
    )(tokens, wa, wo, wb, gain)


def stat_kernel(tensor_size, inner, own_ref, out_ref, slots, send_sem, recv_sem):
    line = lax.axis_index("tensor")
    barrier = pltpu.get_barrier_semaphore()
    for offset in range(1, tensor_size):
        pl.semaphore_signal(
            barrier, inc=1, device_id={"tensor": lax.rem(line + offset, tensor_size)}, device_id_type=MESH
        )
    pl.semaphore_wait(barrier, tensor_size - 1)
    copies = [
        remote(
            own_ref, slots.at[offset], send_sem.at[offset], recv_sem.at[offset],
            {"tensor": lax.rem(line + offset, tensor_size)},
        )
        for offset in range(1, tensor_size)
    ]
    for copy in copies:
        copy.start()
    total = own_ref[...]
    for offset, copy in enumerate(copies, 1):
        copy.wait_recv()
        total = total + slots[offset]
    out_ref[...] = total if inner is None else lax.rsqrt(total / inner + EPSILON)
    for copy in copies:
        copy.wait_send()


def stat_sum(tensor_size, inner, own, identity):
    vmem = pl.BlockSpec(memory_space=pltpu.VMEM)
    dma = pltpu.SemaphoreType.DMA
    return pl.pallas_call(
        functools.partial(stat_kernel, tensor_size, inner),
        in_specs=[vmem],
        out_specs=vmem,
        out_shape=jax.ShapeDtypeStruct(own.shape, F32),
        scratch_shapes=[pltpu.VMEM((tensor_size,) + own.shape, F32), dma((tensor_size,)), dma((tensor_size,))],
        compiler_params=pltpu.CompilerParams(collective_id=identity, has_side_effects=True),
        name="dot_sum" if inner is None else "rms_sum",
    )(own)


BAND = 16


def add_rows(target, terms, count):
    def step(index, carry):
        at = pl.multiple_of(index * BAND, BAND)
        total = terms[0](at)
        for term in terms[1:]:
            total = total + term(at)
        target(at, total)
        return carry

    lax.fori_loop(0, count // BAND, step, 0)


def exit_kernel(
    tensor_size, dp_size,
    ga_ref, go_ref, small_ref,
    sa_ref, so_ref, sb_ref, plane_sum_ref, all_sum_ref,
    near_a, near_o, far_a, far_o, mid_b, b_slots, pair_ref, line_ref, plane_slots, line_slots,
    near_send, near_recv, far_send, far_recv,
    b_send, b_recv, plane_send, plane_recv, line_send, line_recv,
):
    line, plane = lax.axis_index("tensor"), lax.axis_index("dp")
    core, chip, chips = lax.rem(plane, 2), plane // 2, dp_size // 2
    relay = chips == 4
    sibling = {"dp": plane + 1 - 2 * core}
    greet(tensor_size, dp_size)

    grads = [(ga_ref, near_a, far_a), (go_ref, near_o, far_o)]
    order = [3, 1, 2, 0] if relay else list(range(1, chips)) + [0]
    arrays = (0, 1)

    def device(offset, side):
        return 2 * flip(chip, offset) + side

    def near_copy(which, offset):
        grad, near, _ = grads[which]
        return remote(
            grad.at[rows_at(device(offset, 1 - core), near.shape[1])], near.at[offset],
            near_send.at[which, offset], near_recv.at[which, offset], sibling,
        )

    def far_copy(which, offset, half, towards):
        _, near, far = grads[which]
        span = pl.ds(half * (near.shape[1] // 2), near.shape[1] // 2)
        return remote(
            near.at[offset, span], far.at[offset, span],
            far_send.at[which, offset, half], far_recv.at[which, offset, half], {"dp": device(towards, core)},
        )

    def small_plane(offset):
        if offset == 0:
            return remote(small_ref, plane_slots.at[0], plane_send.at[0], plane_recv.at[0], sibling)
        return remote(
            pair_ref, plane_slots.at[offset], plane_send.at[offset], plane_recv.at[offset],
            {"dp": device(offset, core)},
        )

    def small_line(offset):
        return remote(
            line_ref, line_slots.at[offset], line_send.at[offset], line_recv.at[offset],
            {"tensor": lax.rem(line + offset, tensor_size)},
        )

    def near_sum(offset):
        owner = device(offset, core)
        for which in arrays:
            grad, near, _ = grads[which]
            near_copy(which, offset).wait_recv()
            base = owner * near.shape[1]

            def both(at, near=near, grad=grad, base=base):
                mine = grad[pl.ds(pl.multiple_of(base + at, BAND), BAND), :]
                return near[offset, pl.ds(at, BAND), :].astype(F32) + mine.astype(F32)

            def put(at, total, near=near):
                near[offset, pl.ds(at, BAND), :] = total.astype(BF16)

            add_rows(put, [both], near.shape[1])

    def merge(offset, half, source):
        for which in arrays:
            _, near, far = grads[which]
            span = near.shape[1] // 2
            far_copy(which, 3, half, source).wait_recv()

            def both(at, near=near, far=far, span=span):
                at = half * span + at
                return near[offset, pl.ds(at, BAND), :].astype(F32) + far[3, pl.ds(at, BAND), :].astype(F32)

            def put(at, total, near=near, span=span):
                near[offset, pl.ds(half * span + at, BAND), :] = total.astype(BF16)

            add_rows(put, [both], span)
            far_copy(which, offset, half, offset).start()

    for which in arrays:
        near_copy(which, order[0]).start()
    small_plane(0).start()
    for offset in order[1:]:
        for which in arrays:
            near_copy(which, offset).start()

    for offset in order[:-1]:
        near_sum(offset)
        for which in arrays:
            if not relay:
                far_copy(which, offset, 0, offset).start()
                far_copy(which, offset, 1, offset).start()
            elif offset == 3:
                far_copy(which, 3, 0, 1).start()
                far_copy(which, 3, 1, 2).start()
            else:
                far_copy(which, offset, offset - 1, offset).start()
        if offset == order[0]:
            small_plane(0).wait_recv()
            pair_ref[...] = small_ref[...] + plane_slots[0]
            for away in range(1, chips):
                small_plane(away).start()
    near_sum(0)
    if relay:
        merge(1, 1, 2)
        merge(2, 0, 1)
    total = pair_ref[...]
    for offset in range(1, chips):
        small_plane(offset).wait_recv()
        total = total + plane_slots[offset]
    plane_sum_ref[...] = total
    lanes = line_ref.shape[1]
    line_ref[...] = jnp.zeros_like(line_ref)
    for piece in range(4):
        line_ref[piece : piece + 1] = total[8:9, piece * lanes : (piece + 1) * lanes]
    line_ref[4:9, : 2 * STATE] = total[9:14, : 2 * STATE]
    for offset in range(1, tensor_size):
        small_line(offset).start()

    direct = (1, 2) if relay else tuple(range(1, chips))
    block = sb_ref.shape[0]
    for which, out in ((0, sa_ref), (1, so_ref)):
        _, near, far = grads[which]
        for offset in direct:
            for half in (0, 1):
                far_copy(which, offset, half, offset).wait_recv()
        terms = [lambda at, near=near: near[0, pl.ds(at, BAND), :].astype(F32)] + [
            lambda at, far=far, offset=offset: far[offset, pl.ds(at, BAND), :].astype(F32) for offset in direct
        ]

        def put(at, total, out=out):
            out[pl.ds(at, BAND), :] = total

        add_rows(put, terms, near.shape[1])
        if which == 0:
            wide = sb_ref.shape[1]
            own_b = sa_ref.shape[0] // tensor_size
            for j in range(tensor_size):
                mid_b[pl.ds(j * block, own_b), :] = sa_ref[
                    pl.ds(j * own_b, own_b), sa_ref.shape[1] - wide :
                ].astype(BF16)
            b_copies = [
                remote(
                    mid_b.at[rows_at(lax.rem(line + offset, tensor_size), block)], b_slots.at[offset],
                    b_send.at[offset], b_recv.at[offset], {"tensor": lax.rem(line + offset, tensor_size)},
                )
                for offset in range(1, tensor_size)
            ]
            for copy in b_copies:
                copy.start()

    total = line_ref[...]
    for offset in range(1, tensor_size):
        small_line(offset).wait_recv()
        total = total + line_slots[offset]
    all_sum_ref[...] = total

    total = mid_b[rows_at(line, block), :].astype(F32)
    for offset, copy in enumerate(b_copies, 1):
        copy.wait_recv()
        total = total + b_slots[offset].astype(F32)
    sb_ref[...] = total

    for which in arrays:
        for offset in range(chips):
            near_copy(which, offset).wait_send()
            if offset:
                for half in (0, 1):
                    towards = offset if offset != 3 or not relay else half + 1
                    far_copy(which, offset, half, towards).wait_send()
    for copy in b_copies:
        copy.wait_send()
    for offset in range(chips):
        small_plane(offset).wait_send()
    for offset in range(1, tensor_size):
        small_line(offset).wait_send()


def leave(tensor_size, dp_size, block, wide, ga, go, small):
    vmem = pl.BlockSpec(memory_space=pltpu.VMEM)
    dma = pltpu.SemaphoreType.DMA
    chips = dp_size // 2
    packed_line = (16, small.shape[1] // 4)
    ra, ro = ga.shape[0] // dp_size, go.shape[0] // dp_size
    slots = lambda n, r, c, t=BF16: pltpu.VMEM((n, r, c), t)
    return pl.pallas_call(
        functools.partial(exit_kernel, tensor_size, dp_size),
        in_specs=[vmem] * 3,
        out_specs=[vmem] * 5,
        out_shape=[
            jax.ShapeDtypeStruct((ra, ga.shape[1]), F32),
            jax.ShapeDtypeStruct((ro, go.shape[1]), F32),
            jax.ShapeDtypeStruct((block, wide), F32),
            jax.ShapeDtypeStruct(small.shape, F32),
            jax.ShapeDtypeStruct(packed_line, F32),
        ],
        scratch_shapes=[
            slots(chips, ra, ga.shape[1]), slots(chips, ro, go.shape[1]),
            slots(chips, ra, ga.shape[1]), slots(chips, ro, go.shape[1]),
            pltpu.VMEM((tensor_size * block, wide), BF16), slots(tensor_size, block, wide),
            pltpu.VMEM(small.shape, F32), pltpu.VMEM(packed_line, F32),
            slots(chips, *small.shape, F32), slots(tensor_size, *packed_line, F32),
            dma((2, chips)), dma((2, chips)), dma((2, chips, 2)), dma((2, chips, 2)),
            dma((tensor_size,)), dma((tensor_size,)), dma((chips,)), dma((chips,)),
            dma((tensor_size,)), dma((tensor_size,)),
        ],
        compiler_params=pltpu.CompilerParams(collective_id=2, has_side_effects=True, vmem_limit_bytes=60 * MIB),
        name="exit_reduce",
    )(ga, go, small)


STEPS = 4


def finish_kernel(
    width, bc_rows,
    tok_ref, cot_ref, gain_ref, mixed_ref, d_own_ref, sa_ref, dt_ref, sb_ref, plane_ref, all_ref,
    layer_ref, dtok_ref, gzx_ref, gbc_ref, gdt_ref, cxw_ref, cxb_ref, cbw_ref, cbb_ref, dtb_ref, alog_ref, skip_ref,
    gate_ref,
):
    gain = gain_ref[...]

    def step(index, carry):
        at = pl.ds(pl.multiple_of(index * BAND, BAND), BAND)
        tokens = tok_ref[at, :].astype(F32)
        layer_ref[at, :] = (tokens + mixed_ref[at, :].astype(F32)).astype(BF16)
        inv = lax.rsqrt(jnp.mean(tokens * tokens, -1, keepdims=True) + EPSILON)
        d_own = d_own_ref[at, :].astype(F32)
        slope = gain * d_own
        dtok_ref[at, :] = cot_ref[at, :].astype(F32) + (
            inv * slope - tokens * (inv * inv * inv) * jnp.mean(tokens * slope, -1, keepdims=True)
        )
        return carry

    lax.fori_loop(0, tok_ref.shape[0] // BAND, step, 0)
    gzx_ref[:, 0, :] = sa_ref[:, :width]
    gzx_ref[:, 1, :] = sa_ref[:, width : 2 * width]

    @pl.when(pl.program_id(0) == 0)
    def _():
        gbc_ref[...] = sb_ref[:bc_rows]
        heads = dtb_ref.shape[1]
        gdt_ref[...] = dt_ref[...].T[:heads]
        cxw_ref[...] = plane_ref[:4, :width]
        for i in range(width // LANES):
            cxb_ref[i : i + 1] = plane_ref[4:5, i * LANES : (i + 1) * LANES]
            gate_ref[i : i + 1] = plane_ref[5:6, i * LANES : (i + 1) * LANES]
        dtb_ref[...] = plane_ref[6:7, :heads]
        alog_ref[...] = plane_ref[6:7, LANES : LANES + heads]
        cbw_ref[...] = all_ref[4:8, : 2 * STATE]
        cbb_ref[...] = all_ref[8:9, : 2 * STATE]
        per_head = gather_heads(jnp.broadcast_to(plane_ref[7:8, :width], (8, width)), head_expand(width))
        skip_ref[...] = per_head[0:1, :heads]


def finish(width, bc_rows, heads, tokens, cotangent, gain, mixed, d_own, sa, sb, plane_sum, all_sum):
    row = lambda a: pl.BlockSpec((a[0] // STEPS,) + a[1:], lambda i: (i,) + (0,) * (len(a) - 1))
    last = lambda a: pl.BlockSpec((a[0], LANES), lambda i: (0, 2 * width // LANES))
    fixed = lambda a: pl.BlockSpec(a, lambda i: (0, 0))
    shapes = [
        (tokens.shape, BF16), (tokens.shape, F32), ((sa.shape[0], 2, width), F32), ((bc_rows, sb.shape[1]), F32),
        ((heads, sa.shape[0]), F32), ((4, width), F32), ((width // LANES, LANES), F32), ((4, 2 * STATE), F32), ((1, 2 * STATE), F32),
        ((1, heads), F32), ((1, heads), F32), ((1, heads), F32), ((width // LANES, LANES), F32),
    ]
    kinds = [row, row, row] + [fixed] * 10
    args = (tokens, cotangent, gain, mixed, d_own, sa, sa, sb, plane_sum, all_sum)
    inputs = [row, row, fixed, row, row, row, last, fixed, fixed, fixed]
    return pl.pallas_call(
        functools.partial(finish_kernel, width, bc_rows),
        grid=(STEPS,),
        in_specs=[kind(a.shape) for kind, a in zip(inputs, args)],
        out_specs=[kind(s[0]) for kind, s in zip(kinds, shapes)],
        out_shape=[jax.ShapeDtypeStruct(*s) for s in shapes],
        compiler_params=pltpu.CompilerParams(vmem_limit_bytes=61 * MIB),
        name="finish",
    )(*args)


def pad_lanes(values, size):
    return jnp.pad(values, [(0, 0)] * (values.ndim - 1) + [(0, size - values.shape[-1])])


def dot(a, b, dims, out=F32):
    return lax.dot_general(a, b, (dims, ((), ())), preferred_element_type=out)


def body(
    tensor_size, dp_size,
    tokens, segment_ids, cotangent, norm_gain, w_zx, w_bc, w_dt, conv_x_w, conv_x_b, conv_bc_w, conv_bc_b,
    dt_bias, a_log, d_skip, gate_gain, w_out,
):
    own_rows, model = tokens.shape
    weight_rows, _, width = w_zx.shape
    heads_here = w_dt.shape[1]
    inner = width * tensor_size
    bc_rows = w_bc.shape[0]
    bc_padded = -(-bc_rows // 16) * 16
    assert segment_ids.shape[0] == 1

    wa = jnp.concatenate([w_zx.reshape(weight_rows, 2 * width), pad_lanes(w_dt, LANES)], 1)
    wo = w_out.T
    wb = jnp.pad(w_bc, ((0, bc_padded - bc_rows), (0, 0)))
    gain_block = jnp.broadcast_to(pad_lanes(norm_gain[None], LANES), (16, LANES))
    tok_all, wa_all, wo_all, wb_all, gain_all = entry(tensor_size, dp_size, tokens, wa, wo, wb, gain_block)
    cot_late, _ = lax.optimization_barrier((cotangent, gain_all))
    d_out = lax.all_gather(cot_late, "tensor", axis=0, tiled=True)

    gain = gain_all[:, :, 0, : norm_gain.shape[0]].reshape(1, model).astype(F32)
    wb_all = wb_all[:, :, :bc_rows].reshape(model, 2 * STATE)
    meta, meta_next, seg_row = token_meta(segment_ids[0])
    channels = width + 2 * STATE
    params = jnp.concatenate(
        [
            jnp.concatenate([conv_x_w, conv_bc_w], 1),
            jnp.concatenate([conv_x_b, conv_bc_b])[None],
            pad_lanes(dt_bias[None], channels),
            pad_lanes(-jnp.exp(a_log)[None], channels),
            pad_lanes(jnp.repeat(d_skip, HEAD_DIM)[None], channels),
            pad_lanes(gate_gain[None], channels),
            jnp.zeros((7, channels), F32),
        ],
        0,
    )

    x_all = tok_all.astype(F32)
    inv_all = lax.rsqrt(jnp.mean(x_all * x_all, -1, keepdims=True) + EPSILON)
    normed_in = (x_all * inv_all * gain).astype(BF16)
    projected = dot(normed_in, wa_all, ((1,), (0,)))
    bc_pre = dot(normed_in, wb_all, ((1,), (0,)))
    core, gated, states, sums, pre, lanes, small_save = ssm_forward(projected, bc_pre, meta, seg_row, params)

    gate_row = gate_gain[None]
    rms = stat_sum(tensor_size, inner, sums[:1], 1)
    normed_out = (gated * rms[0][:, None] * gate_row).astype(BF16)
    mixed = dot(normed_out, wo_all, ((1,), (1,)), BF16)
    mixed_own = lax.psum_scatter(mixed, "tensor", scatter_dimension=0, tiled=True)
    weights = jnp.concatenate([wa_all, wb_all], 1)
    d_out, mixed, weights = lax.optimization_barrier((d_out, mixed, weights))
    d_normed = dot(d_out, wo_all, ((1,), (0,)))
    inner_part = jnp.sum(gated * gate_row * d_normed, -1)[None]
    dots = inner_part
    for step in range(1, tensor_size):
        dots = dots + lax.ppermute(inner_part, "tensor", [(i, (i + step) % tensor_size) for i in range(tensor_size)])
    go = dot(d_out, normed_out, ((0,), (0,)), BF16)

    dz, packed = ssm_backward(
        inner, projected, bc_pre, meta, meta_next, seg_row, params, core, d_normed, rms, dots, states, pre, lanes, small_save, model
    )
    part = dot(dz, weights, ((1,), (1,)), BF16)
    ga = dot(normed_in, dz, ((0,), (0,)), BF16)
    gnorm = jnp.sum(part.astype(F32) * x_all * inv_all, 0)[None]
    packed = lax.dynamic_update_slice(packed, gnorm, (8, 0))
    d_own = lax.psum_scatter(part, "tensor", scatter_dimension=0, tiled=True)
    ga, part = lax.optimization_barrier((ga, part))
    sa, so, sb, plane_sum, all_sum = leave(tensor_size, dp_size, bc_padded, 2 * STATE, ga, go, packed)
    layer_out, grad_tokens, gzx, gbc, gdt, cxw, cxb, cbw, cbb, dtb, alog, gsk, ggate = finish(
        width, bc_rows, heads_here, tokens, cotangent, gain, mixed_own, d_own, sa, sb, plane_sum, all_sum
    )
    place = lax.axis_index("dp") * tensor_size + lax.axis_index("tensor")
    own_gain = norm_gain.shape[0]
    return (
        layer_out,
        grad_tokens,
        lax.dynamic_slice(all_sum[:4].reshape(model), (place * own_gain,), (own_gain,)),
        gzx, gbc, gdt.T, cxw, cxb.reshape(width), cbw, cbb[0], dtb[0], alog[0], gsk[0], ggate.reshape(width), so.T,
    )


def solution(mesh):
    in_specs = (
        P(("dp", "tensor"), None),
        P("dp", None),
        P(("dp", "tensor"), None),
        P(("dp", "tensor")),
        P("dp", None, "tensor"),
        P(("dp", "tensor"), None),
        P("dp", "tensor"),
        P(None, "tensor"),
        P("tensor"),
        P(),
        P(),
        P("tensor"),
        P("tensor"),
        P("tensor"),
        P("tensor"),
        P("tensor", "dp"),
    )
    out_specs = (
        P(("dp", "tensor"), None),
        P(("dp", "tensor"), None),
        P(("dp", "tensor")),
        P("dp", None, "tensor"),
        P(("dp", "tensor"), None),
        P("dp", "tensor"),
        P(None, "tensor"),
        P("tensor"),
        P(),
        P(),
        P("tensor"),
        P("tensor"),
        P("tensor"),
        P("tensor"),
        P("tensor", "dp"),
    )
    return jax.shard_map(
        functools.partial(body, mesh.shape["tensor"], mesh.shape["dp"]),
        mesh=mesh, in_specs=in_specs, out_specs=out_specs, check_vma=False,
    )
```

```python
import functools
import jax
import jax.numpy as jnp
from jax import lax
from jax.experimental import pallas as pl
from jax.experimental.pallas import tpu as pltpu
from jax.sharding import PartitionSpec as P

HEAD_DIM = 64
STATE = 128
CHUNK = 128
LANES = 128
HALO = 8
HIGHEST = lax.Precision.HIGHEST
NEGATIVE = -1e30
F32 = jnp.float32
BF16 = jnp.bfloat16


def mm(a, b, dims=((1,), (0,))):
    return lax.dot_general(a, b, (dims, ((), ())), preferred_element_type=F32)


def mm_exact(a, b, dims=((1,), (0,))):
    return lax.dot_general(a, b, (dims, ((), ())), precision=HIGHEST, preferred_element_type=F32)


NT = ((1,), (1,))
TN = ((0,), (0,))


def spread(per_head, expand):
    high = per_head.astype(BF16)
    rest = per_head - high.astype(F32)
    middle = rest.astype(BF16)
    low = (rest - middle.astype(F32)).astype(BF16)
    return mm(high, expand) + (mm(middle, expand) + mm(low, expand))


def gather_heads(values, expand):
    high = values.astype(BF16)
    low = (values - high.astype(F32)).astype(BF16)
    return mm(high, expand, NT) + mm(low, expand, NT)


def head_expand(width):
    rows = lax.broadcasted_iota(jnp.int32, (LANES, width), 0)
    columns = lax.broadcasted_iota(jnp.int32, (LANES, width), 1)
    lower = rows * HEAD_DIM
    return ((columns >= lower) & (columns < lower + HEAD_DIM)).astype(F32).astype(BF16)


def triangle(size):
    rows = lax.broadcasted_iota(jnp.int32, (size, size), 0)
    columns = lax.broadcasted_iota(jnp.int32, (size, size), 1)
    return rows >= columns


def sigmoid(values):
    return 1.0 / (1.0 + jnp.exp(-values))


def softplus(values):
    return jnp.maximum(values, 0.0) + jnp.log(1.0 + jnp.exp(-jnp.abs(values)))


def conv_chunk(window, meta, taps, offset):
    total = offset + taps[0:1] * window[pl.ds(HALO, CHUNK), :]
    for back in (1, 2, 3):
        total = total + taps[back : back + 1] * (
            window[pl.ds(HALO - back, CHUNK), :] * meta[:, back : back + 1]
        )
    return total


def split_pair(values):
    lane = lax.broadcasted_iota(jnp.int32, values.shape, 1)
    zero = jnp.zeros_like(values)
    return jnp.where(lane < HEAD_DIM, values, zero), jnp.where(lane < HEAD_DIM, zero, values)


def decays(dt_pre, heads, meta, lower):
    step = softplus(dt_pre + heads[5:6, :LANES])
    rate = step * heads[6:7, :LANES]
    cumulative = mm_exact(lower, rate)
    return step, cumulative


def forward_kernel(
    gate_ref, conv_ref, bc_ref, dt_ref, meta_ref, seg_row_ref, params_ref,
    core_ref, gated_ref, states_ref, sum_ref, pre_ref, lanes_ref, save_ref,
    window, state,
):
    width = conv_ref.shape[1]
    chunk = pl.program_id(0)

    @pl.when(chunk == 0)
    def _():
        window[pl.ds(0, HALO), :] = jnp.zeros((HALO, window.shape[1]), F32)
        state[...] = jnp.zeros_like(state)

    @pl.when(chunk > 0)
    def _():
        window[pl.ds(0, HALO), :] = window[pl.ds(CHUNK, HALO), :]

    window[pl.ds(HALO, CHUNK), :width] = conv_ref[...]
    window[pl.ds(HALO, CHUNK), width:] = bc_ref[...]
    meta = meta_ref[...]
    pre = conv_chunk(window, meta, params_ref, params_ref[4:5])
    pre_ref[...] = pre
    act = pre * sigmoid(pre)
    mixer_in = act[:, :width]
    input_mat = act[:, width : width + STATE].astype(BF16)
    output_mat = act[:, width + STATE :].astype(BF16)
    below = triangle(CHUNK)
    lower = below.astype(F32)
    visible = below & (meta[:, 5:6] == seg_row_ref[0])
    step, cumulative = decays(dt_ref[...], params_ref, meta, lower)
    cum_rows = cumulative.T
    last = cumulative[CHUNK - 1 : CHUNK]
    expand = head_expand(width)
    step_l = spread(step, expand)
    from_prev_l = spread(jnp.exp(cumulative) * meta[:, 0:1], expand)
    to_end_l = spread(jnp.exp(last - cumulative) * meta[:, 4:5], expand)
    lanes_ref[:, :width] = step_l
    lanes_ref[:, width : 2 * width] = from_prev_l
    lanes_ref[:, 2 * width :] = to_end_l
    save_ref[:, :LANES] = step
    save_ref[:, LANES:] = cumulative
    passing = from_prev_l[CHUNK - 1 : CHUNK]
    weighted = mixer_in * step_l
    weighted_b = weighted.astype(BF16)
    scores = mm(output_mat, input_mat, NT)
    incoming = state[...]
    incoming_b = incoming.astype(BF16)
    states_ref[0] = incoming_b
    before = mm(output_mat, incoming_b) * from_prev_l
    skipped = params_ref[7:8, :width] * mixer_in
    for pair in range(width // LANES):
        mixed = []
        for head in (2 * pair, 2 * pair + 1):
            gap = cumulative[:, head : head + 1] - cum_rows[head : head + 1, :]
            decay = jnp.exp(jnp.where(visible, gap, NEGATIVE))
            mixed.append((decay * scores).astype(BF16))
        first, second = split_pair(weighted_b[:, pair * LANES : (pair + 1) * LANES])
        within = mm(jnp.concatenate(mixed, 1), jnp.concatenate([first, second], 0))
        lanes = slice(pair * LANES, (pair + 1) * LANES)
        core_ref[:, lanes] = within + before[:, lanes] + skipped[:, lanes]
    state[...] = passing * incoming + mm(input_mat, (weighted * to_end_l).astype(BF16), TN)
    gate = gate_ref[...]
    gated = core_ref[...] * (gate * sigmoid(gate))
    gated_ref[...] = gated
    square = gated * gated
    sum_ref[...] = mm_exact(jnp.ones((8, width), F32), square, NT)


def ssm_forward(projected, bc_pre, meta, seg_row, params):
    length, width = projected.shape[0], params.shape[1] - 2 * STATE
    chunks = length // CHUNK
    row = lambda n, at=0: pl.BlockSpec((CHUNK, n), lambda c: (c, at))
    fixed = lambda a: pl.BlockSpec(a.shape, lambda c: (0,) * a.ndim)
    return pl.pallas_call(
        forward_kernel,
        grid=(chunks,),
        in_specs=[
            row(width), row(width, 1), row(2 * STATE), row(LANES, 2 * width // LANES), row(8),
            pl.BlockSpec((1, 1, CHUNK), lambda c: (c, 0, 0)),
            fixed(params),
        ],
        out_specs=[
            row(width), row(width),
            pl.BlockSpec((1, STATE, width), lambda c: (c, 0, 0)),
            pl.BlockSpec((8, CHUNK), lambda c: (0, c)),
            row(width + 2 * STATE), row(3 * width), row(2 * LANES),
        ],
        out_shape=[
            jax.ShapeDtypeStruct((length, width), F32),
            jax.ShapeDtypeStruct((length, width), F32),
            jax.ShapeDtypeStruct((chunks, STATE, width), BF16),
            jax.ShapeDtypeStruct((8, length), F32),
            jax.ShapeDtypeStruct((length, width + 2 * STATE), F32),
            jax.ShapeDtypeStruct((length, 3 * width), F32),
            jax.ShapeDtypeStruct((length, 2 * LANES), F32),
        ],
        scratch_shapes=[
            pltpu.VMEM((CHUNK + HALO, width + 2 * STATE), F32),
            pltpu.VMEM((STATE, width), F32),
        ],
        name="ssm_forward",
    )(projected, projected, bc_pre, projected, meta, seg_row, params)


def backward_kernel(
    inner,
    gate_ref, conv_ref, halo_ref, bc_ref, bc_halo_ref, dt_ref, meta_ref, meta_next_ref, seg_row_ref,
    params_ref, core_ref, d_normed_ref, rms_ref, dots_ref, states_ref, pre_ref, lanes_ref, save_ref,
    dz_ref, packed_ref,
    window, d_window, d_state,
):
    width = conv_ref.shape[1]
    place = pl.program_id(0)
    chunk = pl.num_programs(0) - 1 - place

    @pl.when(place == 0)
    def _():
        d_window[pl.ds(CHUNK, HALO), :] = jnp.zeros((HALO, d_window.shape[1]), F32)
        d_state[...] = jnp.zeros_like(d_state)
        packed_ref[...] = jnp.zeros_like(packed_ref)

    @pl.when(place > 0)
    def _():
        d_window[pl.ds(CHUNK, HALO), :] = d_window[pl.ds(0, HALO), :]

    keep_halo = (chunk > 0).astype(F32)
    window[pl.ds(0, HALO), :width] = halo_ref[...] * keep_halo
    window[pl.ds(0, HALO), width:] = bc_halo_ref[...] * keep_halo
    window[pl.ds(HALO, CHUNK), :width] = conv_ref[...]
    window[pl.ds(HALO, CHUNK), width:] = bc_ref[...]
    meta = meta_ref[...]
    pre = pre_ref[...]
    sig = sigmoid(pre)
    act = pre * sig
    slope = sig * (1.0 + pre * (1.0 - sig))
    mixer_in = act[:, :width]
    input_mat = act[:, width : width + STATE].astype(BF16)
    output_mat = act[:, width + STATE :].astype(BF16)
    below = triangle(CHUNK)
    lower = below.astype(F32)
    visible = below & (meta[:, 5:6] == seg_row_ref[0])
    step, cumulative = save_ref[:, :LANES], save_ref[:, LANES:]
    cum_rows = cumulative.T
    expand = head_expand(width)
    step_l = lanes_ref[:, :width]
    from_prev_l = lanes_ref[:, width : 2 * width]
    to_end_l = lanes_ref[:, 2 * width :]
    passing = from_prev_l[CHUNK - 1 : CHUNK]
    weighted = mixer_in * step_l
    weighted_b = weighted.astype(BF16)
    scores = mm(output_mat, input_mat, NT)

    gate_rms = jnp.broadcast_to(rms_ref[...], (8, CHUNK)).T[:, 0:1]
    inner_dot = jnp.broadcast_to(dots_ref[...], (8, CHUNK)).T[:, 0:1]
    gate = gate_ref[...]
    gate_sig = sigmoid(gate)
    gate_act = gate * gate_sig
    core = core_ref[...]
    gated = core * gate_act
    d_normed = d_normed_ref[...]
    d_gated = gate_rms * params_ref[8:9, :width] * d_normed - gated * (
        (gate_rms * gate_rms * gate_rms) * inner_dot / inner
    )
    packed_ref[5:6, :width] += jnp.sum(d_normed * gated * gate_rms, 0, keepdims=True)
    d_core = d_gated * gate_act
    dz_ref[:, :width] = (d_gated * core * (gate_sig * (1.0 + gate * (1.0 - gate_sig)))).astype(BF16)

    d_core_b = d_core.astype(BF16)
    d_core_r = d_core_b.astype(F32)
    incoming_b = states_ref[0]
    d_outgoing = d_state[...]
    d_outgoing_b = d_outgoing.astype(BF16)
    ended = (weighted * to_end_l).astype(BF16)
    after = mm(input_mat, d_outgoing_b) * to_end_l
    scaled_d = (d_core * from_prev_l).astype(BF16)
    d_output = mm(scaled_d, incoming_b, NT)
    d_input = mm(ended, d_outgoing_b, NT)
    d_scores = jnp.zeros((CHUNK, CHUNK), F32)
    d_weighted_parts = []
    for pair in range(width // LANES):
        lanes = slice(pair * LANES, (pair + 1) * LANES)
        first, second = split_pair(weighted_b[:, lanes])
        d_first, d_second = split_pair(d_core_b[:, lanes])
        both_d = mm(d_core_b[:, lanes], jnp.concatenate([first, second], 0), NT)
        mixed = []
        for side, head in enumerate((2 * pair, 2 * pair + 1)):
            gap = cumulative[:, head : head + 1] - cum_rows[head : head + 1, :]
            decay = jnp.exp(jnp.where(visible, gap, NEGATIVE))
            mixed.append((decay * scores).astype(BF16))
            d_scores = d_scores + both_d[:, side * CHUNK : (side + 1) * CHUNK] * decay
        d_weighted_parts.append(
            mm(jnp.concatenate(mixed, 0), jnp.concatenate([d_first, d_second], 0), TN)
        )
    d_within = jnp.concatenate(d_weighted_parts, 1)
    d_scores_b = d_scores.astype(BF16)
    d_output = d_output + mm(d_scores_b, input_mat)
    d_input = d_input + mm(d_scores_b, output_mat, TN)
    d_weighted = d_within + after

    reached = core - params_ref[7:8, :width] * mixer_in
    near = gather_heads(d_core_r * reached - weighted_b.astype(F32) * d_within, expand)
    far_in = gather_heads(weighted * after, expand)
    carried = jnp.sum(d_outgoing * incoming_b.astype(F32), 0, keepdims=True) * passing
    flow = gather_heads(jnp.broadcast_to(carried, (8, width)), expand)[0:1]
    d_rate = mm_exact(lower, near, TN) + (mm_exact(lower, far_in) - far_in) + flow
    d_step = gather_heads(mixer_in * d_weighted, expand) + d_rate * params_ref[6:7, :LANES]
    slope_dt = sigmoid(dt_ref[...] + params_ref[5:6, :LANES])
    d_dt = d_step * slope_dt
    head_lane = lax.broadcasted_iota(jnp.int32, d_dt.shape, 1) < width // HEAD_DIM
    d_dt = jnp.where(head_lane, d_dt, 0.0)
    dz_ref[:, 2 * width : 2 * width + LANES] = d_dt.astype(BF16)
    packed_ref[6:7, :LANES] += jnp.sum(d_dt, 0, keepdims=True)
    packed_ref[6:7, LANES : 2 * LANES] += jnp.sum(d_rate * (step * params_ref[6:7, :LANES]), 0, keepdims=True)
    packed_ref[7:8, :width] += jnp.sum(d_core * mixer_in, 0, keepdims=True)
    d_state[...] = passing * d_outgoing + mm(output_mat, scaled_d, TN)

    d_mixer = d_weighted * step_l + d_core * params_ref[7:8, :width]
    d_pre_x = d_mixer * slope[:, :width]
    d_pre_b = d_input * slope[:, width : width + STATE]
    d_pre_c = d_output * slope[:, width + STATE :]
    d_window[pl.ds(0, CHUNK), :width] = d_pre_x
    d_window[pl.ds(0, CHUNK), width : width + STATE] = d_pre_b
    d_window[pl.ds(0, CHUNK), width + STATE :] = d_pre_c
    d_pre = d_window[pl.ds(0, CHUNK), :]
    taps_seen = [jnp.sum(d_pre * window[pl.ds(HALO, CHUNK), :], 0, keepdims=True)]
    total = params_ref[0:1] * d_pre
    for back in (1, 2, 3):
        taps_seen.append(
            jnp.sum(d_pre * (window[pl.ds(HALO - back, CHUNK), :] * meta[:, back : back + 1]), 0, keepdims=True)
        )
        total = total + params_ref[back : back + 1] * (
            d_window[pl.ds(back, CHUNK), :] * meta_next_ref[:, back : back + 1]
        )
    dz_ref[:, width : 2 * width] = total[:, :width].astype(BF16)
    dz_ref[:, 2 * width + LANES :] = total[:, width:].astype(BF16)
    taps_seen.append(jnp.sum(d_pre, 0, keepdims=True))
    for place_at, seen in enumerate(taps_seen):
        packed_ref[place_at : place_at + 1, :width] += seen[:, :width]
        packed_ref[9 + place_at : 10 + place_at, : 2 * STATE] += seen[:, width:]


def ssm_backward(
    inner, projected, bc_pre, meta, meta_next, seg_row, params, core, d_normed, rms, dots, states,
    pre, lanes, save, model,
):
    length, width = core.shape
    chunks = length // CHUNK
    back = lambda c: chunks - 1 - c
    row = lambda n, at=0: pl.BlockSpec((CHUNK, n), lambda c: (back(c), at))
    fixed = lambda a: pl.BlockSpec(a.shape, lambda c: (0,) * a.ndim)
    ahead = lambda n, at=0: pl.BlockSpec(
        (HALO, n), lambda c: (jnp.maximum(back(c) * (CHUNK // HALO) - 1, 0), at)
    )
    whole = lambda *s: pl.BlockSpec(s, lambda c: (0, 0))
    channels = width + 2 * STATE
    return pl.pallas_call(
        functools.partial(backward_kernel, inner),
        grid=(chunks,),
        in_specs=[
            row(width), row(width, 1), ahead(width, 1), row(2 * STATE), ahead(2 * STATE),
            row(LANES, 2 * width // LANES), row(8), row(8),
            pl.BlockSpec((1, 1, CHUNK), lambda c: (back(c), 0, 0)),
            fixed(params),
            row(width), row(width),
            pl.BlockSpec((1, CHUNK), lambda c: (0, back(c))), pl.BlockSpec((1, CHUNK), lambda c: (0, back(c))),
            pl.BlockSpec((1, STATE, width), lambda c: (back(c), 0, 0)),
            row(channels), row(3 * width), row(2 * LANES),
        ],
        out_specs=[
            row(2 * width + LANES + 2 * STATE), whole(16, model),
        ],
        out_shape=[
            jax.ShapeDtypeStruct((length, 2 * width + LANES + 2 * STATE), BF16),
            jax.ShapeDtypeStruct((16, model), F32),
        ],
        scratch_shapes=[
            pltpu.VMEM((CHUNK + HALO, channels), F32),
            pltpu.VMEM((CHUNK + HALO, channels), F32),
            pltpu.VMEM((STATE, width), F32),
        ],
        name="ssm_backward",
    )(projected, projected, projected, bc_pre, bc_pre, projected, meta, meta_next, seg_row, params,
      core, d_normed, rms, dots, states, pre, lanes, save)


def token_meta(segment):
    length = segment.shape[0]
    chunks = length // CHUNK
    by_chunk = segment.reshape(chunks, CHUNK)
    final = by_chunk[:, -1:]
    ahead = jnp.concatenate([jnp.full((1, 1), -1, jnp.int32), final[:-1]], 0)
    from_prev = (by_chunk == ahead).reshape(length)
    keep_end = (by_chunk == final).reshape(length)
    padded = jnp.concatenate([jnp.full((3,), -1, jnp.int32), segment, jnp.full((3,), -1, jnp.int32)])
    behind = [padded[3 - k : 3 - k + length] == segment for k in (1, 2, 3)]
    after = [padded[3 + k : 3 + k + length] == segment for k in (1, 2, 3)]
    none = jnp.zeros((length,), F32)
    stack = lambda columns: jnp.stack([c.astype(F32) for c in columns], 1)
    meta = stack([from_prev] + behind + [keep_end, segment, none, none])
    meta_next = stack([none] + after + [none] * 4)
    return meta, meta_next, segment.astype(F32).reshape(chunks, 1, CHUNK)


MESH = pl.DeviceIdType.MESH
EPSILON = 1e-05
MIB = 1 << 20


def remote(source, target, send_sem, recv_sem, where):
    return pltpu.make_async_remote_copy(
        src_ref=source, dst_ref=target, send_sem=send_sem, recv_sem=recv_sem, device_id=where, device_id_type=MESH
    )


def rows_at(index, count):
    return pl.ds(pl.multiple_of(index * count, 16), count)


def greet(tensor_size, dp_size):
    line, plane = lax.axis_index("tensor"), lax.axis_index("dp")
    barrier = pltpu.get_barrier_semaphore()
    for step in range(1, tensor_size):
        pl.semaphore_signal(
            barrier, inc=1, device_id={"tensor": lax.rem(line + step, tensor_size)}, device_id_type=MESH
        )
    for step in range(1, dp_size):
        pl.semaphore_signal(barrier, inc=1, device_id={"dp": lax.rem(plane + step, dp_size)}, device_id_type=MESH)
    pl.semaphore_wait(barrier, tensor_size - 1 + dp_size - 1)


def flip(index, offset):
    bit = 1
    while bit <= offset:
        if offset & bit:
            index = index + bit - 2 * bit * lax.rem(index // bit, 2)
        bit *= 2
    return index


def entry_kernel(
    tensor_size, dp_size,
    tok_ref, wa_ref, wo_ref, wb_ref, gain_row_ref, tok_all, wa_all, wo_all, wb_all, gain_all,
    gain_ref, own_sem, right_send, right_recv, left_send, left_recv,
    plane_send, plane_recv, half_send, half_recv, pass_send, pass_recv, small_send, small_recv,
):
    line, plane = lax.axis_index("tensor"), lax.axis_index("dp")
    core, chip, chips = lax.rem(plane, 2), plane // 2, dp_size // 2
    relay = chips == 4
    direct = (1, 2) if relay else tuple(range(1, chips))
    sibling = {"dp": plane + 1 - 2 * core}
    count = tok_ref.shape[0] // PIECES
    smalls = ((wb_ref, wb_all), (gain_ref, gain_all))
    gain_ref[...] = jnp.zeros_like(gain_ref)
    gain_ref[0:1, : gain_row_ref.shape[1]] = gain_row_ref[...].astype(F32)
    greet(tensor_size, dp_size)

    def small_out(which, offset):
        source, place = smalls[which]
        return remote(
            source, place.at[plane, line], small_send.at[which, offset], small_recv.at[which, offset],
            {"tensor": lax.rem(line + offset, tensor_size)},
        )

    for which in (0, 1):
        for offset in range(1, tensor_size):
            small_out(which, offset).start()
    own = [
        pltpu.make_async_copy(wb_ref, wb_all.at[plane, line], own_sem.at[0]),
        pltpu.make_async_copy(gain_ref, gain_all.at[plane, line], own_sem.at[1]),
        pltpu.make_async_copy(tok_ref, tok_all.at[rows_at(line, tok_ref.shape[0])], own_sem.at[2]),
        pltpu.make_async_copy(wa_ref, wa_all.at[rows_at(plane, wa_ref.shape[0])], own_sem.at[3]),
        pltpu.make_async_copy(wo_ref, wo_all.at[rows_at(plane, wo_ref.shape[0])], own_sem.at[4]),
    ]

    def token_copy(step, piece, to_right, arriving=False):
        origin = line - step if to_right else line + step
        if arriving:
            origin = origin - 1 if to_right else origin + 1
        origin = jnp.clip(origin, 0, tensor_size - 1)
        place = tok_all.at[rows_at(origin * PIECES + piece, count)]
        source = tok_ref.at[pl.ds(piece * count, count)] if step == 0 and not arriving else place
        neighbour = line + 1 if to_right != arriving else line - 1
        return remote(
            source, place,
            (right_send if to_right else left_send).at[step, piece],
            (right_recv if to_right else left_recv).at[step, piece],
            {"tensor": jnp.clip(neighbour, 0, tensor_size - 1)},
        )

    def sends(step, to_right):
        if to_right:
            return (line - step >= 0) & (line + 1 < tensor_size)
        return (line + step < tensor_size) & (line >= 1)

    def forward_tokens(step):
        for piece in range(PIECES):
            for to_right in (True, False):
                @pl.when(sends(step, to_right))
                def _():
                    if step > 0:
                        token_copy(step - 1, piece, to_right, True).wait_recv()
                    token_copy(step, piece, to_right).start()

    def shard(ref, source):
        rows = source.shape[0]
        return lambda d, half=None: ref.at[
            rows_at(d, rows) if half is None else pl.ds(pl.multiple_of(d * rows + half * (rows // 2), 16), rows // 2)
        ]

    def block(ref):
        n = ref.shape[1] // 2
        return lambda d, half=None: ref.at[d] if half is None else ref.at[d, pl.ds(half * n, n)]

    stacks = [
        (wo_ref, shard(wo_all, wo_ref)),
        (None, block(wb_all)),
        (None, block(gain_all)),
        (wa_ref, shard(wa_all, wa_ref)),
    ]

    def device(offset, side):
        return 2 * flip(chip, offset) + side

    def plane_copy(which, offset):
        source, place = stacks[which]
        return remote(
            place(plane) if source is None else source, place(plane),
            plane_send.at[which, offset], plane_recv.at[which, offset], {"dp": device(offset, core)},
        )

    def plane_arrival(which, offset):
        origin = device(offset, core)
        place = stacks[which][1](origin)
        return remote(place, place, plane_send.at[which, offset], plane_recv.at[which, offset], {"dp": origin})

    def half_copy(which, half):
        place = stacks[which][1](device(half + 1, core), half)
        return remote(
            place, place, half_send.at[which, half], half_recv.at[which, half], {"dp": device(2 - half, core)}
        )

    def half_arrival(which, half):
        place = stacks[which][1](device(3, core), half)
        return remote(
            place, place, half_send.at[which, half], half_recv.at[which, half], {"dp": device(2 - half, core)}
        )

    def pass_copy(which, offset, arriving=False):
        source, place = stacks[which]
        origin = device(offset, 1 - core if arriving else core)
        return remote(
            source if offset == 0 and source is not None and not arriving else place(origin), place(origin),
            pass_send.at[which, offset], pass_recv.at[which, offset], sibling,
        )

    def plane_start(which):
        for offset in direct:
            plane_copy(which, offset).start()

    def plane_next(which):
        for offset in direct:
            plane_arrival(which, offset).wait_recv()
            if relay:
                half_copy(which, offset - 1).start()
            pass_copy(which, offset).start()

    def plane_last(which):
        if relay:
            half_arrival(which, 0).wait_recv()
            half_arrival(which, 1).wait_recv()
            pass_copy(which, 3).start()

    forward_tokens(0)
    plane_start(0)
    for copy in own:
        copy.start()
    own[0].wait()
    own[1].wait()
    for which in (0, 1):
        for offset in range(1, tensor_size):
            small_out(which, offset).wait_recv()
    plane_start(1)
    plane_start(2)
    plane_start(3)
    for which in range(4):
        pass_copy(which, 0).start()
    plane_next(0)
    plane_next(1)
    plane_next(2)
    forward_tokens(1)
    plane_next(3)
    for which in range(3):
        plane_last(which)
    for step in range(2, tensor_size - 1):
        forward_tokens(step)
    plane_last(3)

    for to_right in (True, False):
        for step in range(tensor_size - 1):
            arrives = line - 1 - step >= 0 if to_right else line + 1 + step < tensor_size
            at_end = line + 1 == tensor_size if to_right else line == 0

            @pl.when(arrives & at_end)
            def _():
                for piece in range(PIECES):
                    token_copy(step, piece, to_right, True).wait_recv()

            @pl.when(sends(step, to_right))
            def _():
                for piece in range(PIECES):
                    token_copy(step, piece, to_right).wait_send()

    for which in range(4):
        for offset in range(chips):
            pass_copy(which, offset, True).wait_recv()
            pass_copy(which, offset).wait_send()
        for offset in direct:
            plane_copy(which, offset).wait_send()
        if relay:
            half_copy(which, 0).wait_send()
            half_copy(which, 1).wait_send()
    for which in (0, 1):
        for offset in range(1, tensor_size):
            small_out(which, offset).wait_send()
    for copy in own[2:]:
        copy.wait()


PIECES = 2


def entry(tensor_size, dp_size, tokens, wa, wo, wb, gain):
    vmem = pl.BlockSpec(memory_space=pltpu.VMEM)
    anywhere = pl.BlockSpec(memory_space=pl.ANY)
    dma = pltpu.SemaphoreType.DMA
    chips = dp_size // 2
    return pl.pallas_call(
        functools.partial(entry_kernel, tensor_size, dp_size),
        in_specs=[vmem] * 5,
        out_specs=[anywhere] * 5,
        out_shape=[
            jax.ShapeDtypeStruct((tensor_size * tokens.shape[0], tokens.shape[1]), BF16),
            jax.ShapeDtypeStruct((dp_size * wa.shape[0], wa.shape[1]), BF16),
            jax.ShapeDtypeStruct((dp_size * wo.shape[0], wo.shape[1]), BF16),
            jax.ShapeDtypeStruct((dp_size, tensor_size) + wb.shape, BF16),
            jax.ShapeDtypeStruct((dp_size, tensor_size, 8, LANES), F32),
        ],
        scratch_shapes=[
            pltpu.VMEM((8, LANES), F32), dma((5,)), *[dma((tensor_size, PIECES))] * 4,
            dma((4, chips)), dma((4, chips)), dma((4, 2)), dma((4, 2)), dma((4, chips)), dma((4, chips)),
            dma((2, tensor_size)), dma((2, tensor_size)),
        ],
        compiler_params=pltpu.CompilerParams(collective_id=0, has_side_effects=True),
        name="entry_gather",
    )(tokens, wa, wo, wb, gain)


def stat_kernel(tensor_size, inner, own_ref, out_ref, slots, send_sem, recv_sem):
    line = lax.axis_index("tensor")
    barrier = pltpu.get_barrier_semaphore()
    for offset in range(1, tensor_size):
        pl.semaphore_signal(
            barrier, inc=1, device_id={"tensor": lax.rem(line + offset, tensor_size)}, device_id_type=MESH
        )
    pl.semaphore_wait(barrier, tensor_size - 1)
    copies = [
        remote(
            own_ref, slots.at[offset], send_sem.at[offset], recv_sem.at[offset],
            {"tensor": lax.rem(line + offset, tensor_size)},
        )
        for offset in range(1, tensor_size)
    ]
    for copy in copies:
        copy.start()
    total = own_ref[...]
    for offset, copy in enumerate(copies, 1):
        copy.wait_recv()
        total = total + slots[offset]
    out_ref[...] = total if inner is None else lax.rsqrt(total / inner + EPSILON)
    for copy in copies:
        copy.wait_send()


def stat_sum(tensor_size, inner, own, identity):
    vmem = pl.BlockSpec(memory_space=pltpu.VMEM)
    dma = pltpu.SemaphoreType.DMA
    return pl.pallas_call(
        functools.partial(stat_kernel, tensor_size, inner),
        in_specs=[vmem],
        out_specs=vmem,
        out_shape=jax.ShapeDtypeStruct(own.shape, F32),
        scratch_shapes=[pltpu.VMEM((tensor_size,) + own.shape, F32), dma((tensor_size,)), dma((tensor_size,))],
        compiler_params=pltpu.CompilerParams(collective_id=identity, has_side_effects=True),
        name="dot_sum" if inner is None else "rms_sum",
    )(own)


BAND = 16


def add_rows(target, terms, count):
    def step(index, carry):
        at = pl.multiple_of(index * BAND, BAND)
        total = terms[0](at)
        for term in terms[1:]:
            total = total + term(at)
        target(at, total)
        return carry

    lax.fori_loop(0, count // BAND, step, 0)


def exit_kernel(
    tensor_size, dp_size,
    ga_ref, go_ref, small_ref,
    sa_ref, so_ref, sb_ref, plane_sum_ref, all_sum_ref,
    near_a, near_o, far_a, far_o, mid_b, b_slots, pair_ref, line_ref, plane_slots, line_slots,
    near_send, near_recv, far_send, far_recv,
    b_send, b_recv, plane_send, plane_recv, line_send, line_recv,
):
    line, plane = lax.axis_index("tensor"), lax.axis_index("dp")
    core, chip, chips = lax.rem(plane, 2), plane // 2, dp_size // 2
    relay = chips == 4
    sibling = {"dp": plane + 1 - 2 * core}
    greet(tensor_size, dp_size)

    grads = [(ga_ref, near_a, far_a), (go_ref, near_o, far_o)]
    order = [3, 1, 2, 0] if relay else list(range(1, chips)) + [0]
    arrays = (0, 1)

    def device(offset, side):
        return 2 * flip(chip, offset) + side

    def near_copy(which, offset):
        grad, near, _ = grads[which]
        return remote(
            grad.at[rows_at(device(offset, 1 - core), near.shape[1])], near.at[offset],
            near_send.at[which, offset], near_recv.at[which, offset], sibling,
        )

    def far_copy(which, offset, half, towards):
        _, near, far = grads[which]
        span = pl.ds(half * (near.shape[1] // 2), near.shape[1] // 2)
        return remote(
            near.at[offset, span], far.at[offset, span],
            far_send.at[which, offset, half], far_recv.at[which, offset, half], {"dp": device(towards, core)},
        )

    def small_plane(offset):
        if offset == 0:
            return remote(small_ref, plane_slots.at[0], plane_send.at[0], plane_recv.at[0], sibling)
        return remote(
            pair_ref, plane_slots.at[offset], plane_send.at[offset], plane_recv.at[offset],
            {"dp": device(offset, core)},
        )

    def small_line(offset):
        return remote(
            line_ref, line_slots.at[offset], line_send.at[offset], line_recv.at[offset],
            {"tensor": lax.rem(line + offset, tensor_size)},
        )

    def near_sum(offset):
        owner = device(offset, core)
        for which in arrays:
            grad, near, _ = grads[which]
            near_copy(which, offset).wait_recv()
            base = owner * near.shape[1]

            def both(at, near=near, grad=grad, base=base):
                mine = grad[pl.ds(pl.multiple_of(base + at, BAND), BAND), :]
                return near[offset, pl.ds(at, BAND), :].astype(F32) + mine.astype(F32)

            def put(at, total, near=near):
                near[offset, pl.ds(at, BAND), :] = total.astype(BF16)

            add_rows(put, [both], near.shape[1])

    def merge(offset, half, source):
        for which in arrays:
            _, near, far = grads[which]
            span = near.shape[1] // 2
            far_copy(which, 3, half, source).wait_recv()

            def both(at, near=near, far=far, span=span):
                at = half * span + at
                return near[offset, pl.ds(at, BAND), :].astype(F32) + far[3, pl.ds(at, BAND), :].astype(F32)

            def put(at, total, near=near, span=span):
                near[offset, pl.ds(half * span + at, BAND), :] = total.astype(BF16)

            add_rows(put, [both], span)
            far_copy(which, offset, half, offset).start()

    for which in arrays:
        near_copy(which, order[0]).start()
    small_plane(0).start()
    for offset in order[1:]:
        for which in arrays:
            near_copy(which, offset).start()

    for offset in order[:-1]:
        near_sum(offset)
        for which in arrays:
            if not relay:
                far_copy(which, offset, 0, offset).start()
                far_copy(which, offset, 1, offset).start()
            elif offset == 3:
                far_copy(which, 3, 0, 1).start()
                far_copy(which, 3, 1, 2).start()
            else:
                far_copy(which, offset, offset - 1, offset).start()
        if offset == order[0]:
            small_plane(0).wait_recv()
            pair_ref[...] = small_ref[...] + plane_slots[0]
            for away in range(1, chips):
                small_plane(away).start()
    near_sum(0)
    if relay:
        merge(1, 1, 2)
        merge(2, 0, 1)
    total = pair_ref[...]
    for offset in range(1, chips):
        small_plane(offset).wait_recv()
        total = total + plane_slots[offset]
    plane_sum_ref[...] = total
    lanes = line_ref.shape[1]
    line_ref[...] = jnp.zeros_like(line_ref)
    for piece in range(4):
        line_ref[piece : piece + 1] = total[8:9, piece * lanes : (piece + 1) * lanes]
    line_ref[4:9, : 2 * STATE] = total[9:14, : 2 * STATE]
    for offset in range(1, tensor_size):
        small_line(offset).start()

    direct = (1, 2) if relay else tuple(range(1, chips))
    block = sb_ref.shape[0]
    for which, out in ((0, sa_ref), (1, so_ref)):
        _, near, far = grads[which]
        for offset in direct:
            for half in (0, 1):
                far_copy(which, offset, half, offset).wait_recv()
        terms = [lambda at, near=near: near[0, pl.ds(at, BAND), :].astype(F32)] + [
            lambda at, far=far, offset=offset: far[offset, pl.ds(at, BAND), :].astype(F32) for offset in direct
        ]

        def put(at, total, out=out):
            out[pl.ds(at, BAND), :] = total

        add_rows(put, terms, near.shape[1])
        if which == 0:
            wide = sb_ref.shape[1]
            own_b = sa_ref.shape[0] // tensor_size
            for j in range(tensor_size):
                mid_b[pl.ds(j * block, own_b), :] = sa_ref[
                    pl.ds(j * own_b, own_b), sa_ref.shape[1] - wide :
                ].astype(BF16)
            b_copies = [
                remote(
                    mid_b.at[rows_at(lax.rem(line + offset, tensor_size), block)], b_slots.at[offset],
                    b_send.at[offset], b_recv.at[offset], {"tensor": lax.rem(line + offset, tensor_size)},
                )
                for offset in range(1, tensor_size)
            ]
            for copy in b_copies:
                copy.start()

    total = line_ref[...]
    for offset in range(1, tensor_size):
        small_line(offset).wait_recv()
        total = total + line_slots[offset]
    all_sum_ref[...] = total

    total = mid_b[rows_at(line, block), :].astype(F32)
    for offset, copy in enumerate(b_copies, 1):
        copy.wait_recv()
        total = total + b_slots[offset].astype(F32)
    sb_ref[...] = total

    for which in arrays:
        for offset in range(chips):
            near_copy(which, offset).wait_send()
            if offset:
                for half in (0, 1):
                    towards = offset if offset != 3 or not relay else half + 1
                    far_copy(which, offset, half, towards).wait_send()
    for copy in b_copies:
        copy.wait_send()
    for offset in range(chips):
        small_plane(offset).wait_send()
    for offset in range(1, tensor_size):
        small_line(offset).wait_send()


def leave(tensor_size, dp_size, block, wide, ga, go, small):
    vmem = pl.BlockSpec(memory_space=pltpu.VMEM)
    dma = pltpu.SemaphoreType.DMA
    chips = dp_size // 2
    packed_line = (16, small.shape[1] // 4)
    ra, ro = ga.shape[0] // dp_size, go.shape[0] // dp_size
    slots = lambda n, r, c, t=BF16: pltpu.VMEM((n, r, c), t)
    return pl.pallas_call(
        functools.partial(exit_kernel, tensor_size, dp_size),
        in_specs=[vmem] * 3,
        out_specs=[vmem] * 5,
        out_shape=[
            jax.ShapeDtypeStruct((ra, ga.shape[1]), F32),
            jax.ShapeDtypeStruct((ro, go.shape[1]), F32),
            jax.ShapeDtypeStruct((block, wide), F32),
            jax.ShapeDtypeStruct(small.shape, F32),
            jax.ShapeDtypeStruct(packed_line, F32),
        ],
        scratch_shapes=[
            slots(chips, ra, ga.shape[1]), slots(chips, ro, go.shape[1]),
            slots(chips, ra, ga.shape[1]), slots(chips, ro, go.shape[1]),
            pltpu.VMEM((tensor_size * block, wide), BF16), slots(tensor_size, block, wide),
            pltpu.VMEM(small.shape, F32), pltpu.VMEM(packed_line, F32),
            slots(chips, *small.shape, F32), slots(tensor_size, *packed_line, F32),
            dma((2, chips)), dma((2, chips)), dma((2, chips, 2)), dma((2, chips, 2)),
            dma((tensor_size,)), dma((tensor_size,)), dma((chips,)), dma((chips,)),
            dma((tensor_size,)), dma((tensor_size,)),
        ],
        compiler_params=pltpu.CompilerParams(collective_id=2, has_side_effects=True, vmem_limit_bytes=60 * MIB),
        name="exit_reduce",
    )(ga, go, small)


STEPS = 4


def tokens_kernel(tok_ref, cot_ref, gain_ref, mixed_ref, d_own_ref, layer_ref, dtok_ref):
    gain = gain_ref[...]

    def step(index, carry):
        at = pl.ds(pl.multiple_of(index * BAND, BAND), BAND)
        tokens = tok_ref[at, :].astype(F32)
        layer_ref[at, :] = (tokens + mixed_ref[at, :].astype(F32)).astype(BF16)
        inv = lax.rsqrt(jnp.mean(tokens * tokens, -1, keepdims=True) + EPSILON)
        slope = gain * d_own_ref[at, :].astype(F32)
        dtok_ref[at, :] = cot_ref[at, :].astype(F32) + (
            inv * slope - tokens * (inv * inv * inv) * jnp.mean(tokens * slope, -1, keepdims=True)
        )
        return carry

    lax.fori_loop(0, tok_ref.shape[0] // BAND, step, 0)


def finish_tokens(tokens, cotangent, gain, mixed, d_own):
    row = pl.BlockSpec((tokens.shape[0] // STEPS, tokens.shape[1]), lambda i: (i, 0))
    return pl.pallas_call(
        tokens_kernel,
        grid=(STEPS,),
        in_specs=[row, row, pl.BlockSpec(gain.shape, lambda i: (0, 0)), row, row],
        out_specs=[row, row],
        out_shape=[jax.ShapeDtypeStruct(tokens.shape, BF16), jax.ShapeDtypeStruct(tokens.shape, F32)],
        compiler_params=pltpu.CompilerParams(vmem_limit_bytes=61 * MIB),
        name="finish_tokens",
    )(tokens, cotangent, gain, mixed, d_own)


def weights_kernel(
    width, bc_rows,
    sa_ref, dt_ref, sb_ref, plane_ref, all_ref,
    gzx_ref, gbc_ref, gdt_ref, cxw_ref, cxb_ref, cbw_ref, cbb_ref, dtb_ref, alog_ref, skip_ref, gate_ref,
):
    gzx_ref[:, 0, :] = sa_ref[:, :width]
    gzx_ref[:, 1, :] = sa_ref[:, width : 2 * width]

    @pl.when(pl.program_id(0) == 0)
    def _():
        gbc_ref[...] = sb_ref[:bc_rows]
        heads = dtb_ref.shape[1]
        gdt_ref[...] = dt_ref[...].T[:heads]
        cxw_ref[...] = plane_ref[:4, :width]
        for i in range(width // LANES):
            cxb_ref[i : i + 1] = plane_ref[4:5, i * LANES : (i + 1) * LANES]
            gate_ref[i : i + 1] = plane_ref[5:6, i * LANES : (i + 1) * LANES]
        dtb_ref[...] = plane_ref[6:7, :heads]
        alog_ref[...] = plane_ref[6:7, LANES : LANES + heads]
        cbw_ref[...] = all_ref[4:8, : 2 * STATE]
        cbb_ref[...] = all_ref[8:9, : 2 * STATE]
        per_head = gather_heads(jnp.broadcast_to(plane_ref[7:8, :width], (8, width)), head_expand(width))
        skip_ref[...] = per_head[0:1, :heads]


def finish_weights(width, bc_rows, heads, sa, sb, plane_sum, all_sum):
    row = lambda a: pl.BlockSpec((a[0] // STEPS,) + a[1:], lambda i: (i,) + (0,) * (len(a) - 1))
    last = lambda a: pl.BlockSpec((a[0], LANES), lambda i: (0, 2 * width // LANES))
    fixed = lambda a: pl.BlockSpec(a, lambda i: (0, 0))
    shapes = [
        (sa.shape[0], 2, width), (bc_rows, sb.shape[1]), (heads, sa.shape[0]), (4, width), (width // LANES, LANES),
        (4, 2 * STATE), (1, 2 * STATE), (1, heads), (1, heads), (1, heads), (width // LANES, LANES),
    ]
    args = (sa, sa, sb, plane_sum, all_sum)
    return pl.pallas_call(
        functools.partial(weights_kernel, width, bc_rows),
        grid=(STEPS,),
        in_specs=[kind(a.shape) for kind, a in zip([row, last, fixed, fixed, fixed], args)],
        out_specs=[kind(shape) for kind, shape in zip([row] + [fixed] * 10, shapes)],
        out_shape=[jax.ShapeDtypeStruct(shape, F32) for shape in shapes],
        compiler_params=pltpu.CompilerParams(vmem_limit_bytes=61 * MIB),
        name="finish_weights",
    )(*args)


def pad_lanes(values, size):
    return jnp.pad(values, [(0, 0)] * (values.ndim - 1) + [(0, size - values.shape[-1])])


def dot(a, b, dims, out=F32):
    return lax.dot_general(a, b, (dims, ((), ())), preferred_element_type=out)


def body(
    tensor_size, dp_size,
    tokens, segment_ids, cotangent, norm_gain, w_zx, w_bc, w_dt, conv_x_w, conv_x_b, conv_bc_w, conv_bc_b,
    dt_bias, a_log, d_skip, gate_gain, w_out,
):
    own_rows, model = tokens.shape
    weight_rows, _, width = w_zx.shape
    heads_here = w_dt.shape[1]
    inner = width * tensor_size
    bc_rows = w_bc.shape[0]
    bc_padded = -(-bc_rows // 16) * 16
    assert segment_ids.shape[0] == 1

    wa = jnp.concatenate([w_zx.reshape(weight_rows, 2 * width), pad_lanes(w_dt, LANES)], 1)
    wo = w_out.T
    wb = jnp.pad(w_bc, ((0, bc_padded - bc_rows), (0, 0)))
    tok_all, wa_all, wo_all, wb_all, gain_all = entry(tensor_size, dp_size, tokens, wa, wo, wb, norm_gain[None])
    cot_late, _ = lax.optimization_barrier((cotangent, gain_all))
    d_out = lax.all_gather(cot_late, "tensor", axis=0, tiled=True)

    gain = gain_all[:, :, 0, : norm_gain.shape[0]].reshape(1, model)
    wb_all = wb_all[:, :, :bc_rows].reshape(model, 2 * STATE)
    meta, meta_next, seg_row = token_meta(segment_ids[0])
    channels = width + 2 * STATE
    params = jnp.concatenate(
        [
            jnp.concatenate([conv_x_w, conv_bc_w], 1),
            jnp.concatenate([conv_x_b, conv_bc_b])[None],
            pad_lanes(dt_bias[None], channels),
            pad_lanes(-jnp.exp(a_log)[None], channels),
            pad_lanes(jnp.repeat(d_skip, HEAD_DIM)[None], channels),
            pad_lanes(gate_gain[None], channels),
            jnp.zeros((7, channels), F32),
        ],
        0,
    )

    x_all = tok_all.astype(F32)
    inv_all = lax.rsqrt(jnp.mean(x_all * x_all, -1, keepdims=True) + EPSILON)
    normed_in = (x_all * inv_all * gain).astype(BF16)
    projected = dot(normed_in, wa_all, ((1,), (0,)))
    bc_pre = dot(normed_in, wb_all, ((1,), (0,)))
    core, gated, states, sums, pre, lanes, small_save = ssm_forward(projected, bc_pre, meta, seg_row, params)

    gate_row = gate_gain[None]
    rms = stat_sum(tensor_size, inner, sums[:1], 1)
    normed_out = (gated * rms[0][:, None] * gate_row).astype(BF16)
    mixed = dot(normed_out, wo_all, ((1,), (1,)), BF16)
    mixed_own = lax.psum_scatter(mixed, "tensor", scatter_dimension=0, tiled=True)
    weights = jnp.concatenate([wa_all, wb_all], 1)
    d_out, mixed, weights = lax.optimization_barrier((d_out, mixed, weights))
    d_normed = dot(d_out, wo_all, ((1,), (0,)))
    inner_part = jnp.sum(gated * gate_row * d_normed, -1)[None]
    dots = inner_part
    for step in range(1, tensor_size):
        dots = dots + lax.ppermute(inner_part, "tensor", [(i, (i + step) % tensor_size) for i in range(tensor_size)])
    go = dot(d_out, normed_out, ((0,), (0,)), BF16)

    dots, go = lax.optimization_barrier((dots, go))
    dz, packed = ssm_backward(
        inner, projected, bc_pre, meta, meta_next, seg_row, params, core, d_normed, rms, dots, states, pre, lanes, small_save, model
    )
    part = dot(dz, weights, ((1,), (1,)), BF16)
    ga = dot(normed_in, dz, ((0,), (0,)), BF16)
    gnorm = jnp.sum(part.astype(F32) * x_all * inv_all, 0)[None]
    packed = lax.dynamic_update_slice(packed, gnorm, (8, 0))
    d_own = lax.psum_scatter(part, "tensor", scatter_dimension=0, tiled=True)
    ga, part = lax.optimization_barrier((ga, part))
    sa, so, sb, plane_sum, all_sum = leave(tensor_size, dp_size, bc_padded, 2 * STATE, ga, go, packed)
    gzx, gbc, gdt, cxw, cxb, cbw, cbb, dtb, alog, gsk, ggate = finish_weights(
        width, bc_rows, heads_here, sa, sb, plane_sum, all_sum
    )
    layer_out, grad_tokens = finish_tokens(tokens, cotangent, gain, mixed_own, d_own)
    place = lax.axis_index("dp") * tensor_size + lax.axis_index("tensor")
    own_gain = norm_gain.shape[0]
    return (
        layer_out,
        grad_tokens,
        lax.dynamic_slice(all_sum[:4].reshape(model), (place * own_gain,), (own_gain,)),
        gzx, gbc, gdt.T, cxw, cxb.reshape(width), cbw, cbb[0], dtb[0], alog[0], gsk[0], ggate.reshape(width), so.T,
    )


def solution(mesh):
    in_specs = (
        P(("dp", "tensor"), None),
        P("dp", None),
        P(("dp", "tensor"), None),
        P(("dp", "tensor")),
        P("dp", None, "tensor"),
        P(("dp", "tensor"), None),
        P("dp", "tensor"),
        P(None, "tensor"),
        P("tensor"),
        P(),
        P(),
        P("tensor"),
        P("tensor"),
        P("tensor"),
        P("tensor"),
        P("tensor", "dp"),
    )
    out_specs = (
        P(("dp", "tensor"), None),
        P(("dp", "tensor"), None),
        P(("dp", "tensor")),
        P("dp", None, "tensor"),
        P(("dp", "tensor"), None),
        P("dp", "tensor"),
        P(None, "tensor"),
        P("tensor"),
        P(),
        P(),
        P("tensor"),
        P("tensor"),
        P("tensor"),
        P("tensor"),
        P("tensor", "dp"),
    )
    return jax.shard_map(
        functools.partial(body, mesh.shape["tensor"], mesh.shape["dp"]),
        mesh=mesh, in_specs=in_specs, out_specs=out_specs, check_vma=False,
    )
```
